32 devices in a mesh: pipe: 2 (over core), dp: 8 (over z, y), tensor: 2 (over x).
Axes of the slice: x: 2, y: 2, z: 4, core: 2. Of those that a mesh axis runs over, the one named last changes fastest.
Arguments:
- hidden_in: bfloat16 [2, 16, 2, 64, 3584], P('pipe', 'dp'), may hold values from -60 to 60, as said below
- attention_probs: bfloat16 [2, 16, 2, 14, 64, 64], P('pipe', 'dp', None, 'tensor'), may hold values from 0 to 1, as said below
- norm_gain: float32 [2, 3584], P('pipe'), may hold values from 0.5 to 1.5
- value_weight: bfloat16 [2, 3584, 256], P('pipe', None, 'tensor'), may hold values from -0.09375 to 0.09375
- output_weight: bfloat16 [2, 1792, 3584], P('pipe', 'tensor'), may hold values from -0.125 to 0.125
- head_grad: bfloat16 [16, 2, 64, 3584], P('dp', 'tensor'), may hold values from -16 to 16
- policy_logprob: float32 [16, 2, 64], P('dp'), may hold values from -3 to -0.2
- reference_logprob: float32 [16, 2], P('dp'), may hold values from -96 to -12.8
- sequence_bounds: int32 [16, 3], P('dp'), may hold values from 1 to 64, as said below
Outputs:
- section_cotangent: bfloat16 [2, 16, 2, 64, 3584], P('pipe', 'dp', 'tensor')
- value_gradient: float32 [2, 3584, 256], P('pipe', 'dp', 'tensor')
- output_gradient: float32 [2, 3584, 1792], P('pipe', 'dp', 'tensor')
- gain_gradient: float32 [2, 3584], P('pipe', 'dp')
The draws below stay inside these ranges and needn't reach their ends.
Inputs may be any that keep to these rules, and one draw needn't show every extreme that they name: `sequence_bounds`: entry 0 is the prompt length, shared by the two sequences of a pair; a sequence's response is the positions from entry 0 up to its end (entry 1 for the chosen, entry 2 for the rejected sequence), and holds one position or more. `attention_probs`: each row is a causal attention distribution: zero above the diagonal, summing to one before rounding. `hidden_in`: activations of varying size from token to token.
All inputs are finite; a program needn't handle non-finite values.
Results may differ from the reference program's by a relative error of at most 0.017.
Values may be sent and summed in bfloat16 or wider, within the bound.
A program may use at most 128 MiB of HBM per device.

```python
import math
import jax
import jax.numpy as jnp
from jax import lax

D = 3584
HEADS = 14
KV_HEADS = 2
HEAD_DIM = 128
SEQ = 64
PAIRS = 16
N_PIPE = 2
N_TENSOR = 2


def draw_hidden_in(key, part):
    key_main, key_scale = jax.random.split(key, 2)
    full_shape = (N_PIPE, PAIRS, 2, SEQ, D)
    row_scale = jnp.exp(jax.random.uniform(key_scale, (N_PIPE, PAIRS, 2, SEQ, 1), jnp.float32, 0.0, math.log(10.0)))
    noise = jnp.clip(jax.random.normal(key_main, full_shape, jnp.float32), -6.0, 6.0)
    return (row_scale * noise).astype(jnp.bfloat16)


def draw_attention_probs(key, part):
    key_noise, key_temper, key_slope = jax.random.split(key, 3)
    full_shape = (N_PIPE, PAIRS, 2, HEADS, SEQ, SEQ)
    head_shape = (N_PIPE, 1, 1, HEADS, 1, 1)
    temper = jnp.exp(jax.random.uniform(key_temper, head_shape, jnp.float32, math.log(0.5), math.log(3.0)))
    decay_slope = jnp.exp(jax.random.uniform(key_slope, head_shape, jnp.float32, math.log(0.5 / SEQ), 0.0))
    query_pos = jnp.arange(SEQ)[:, None]
    key_pos = jnp.arange(SEQ)[None, :]
    distance = (query_pos - key_pos).astype(jnp.float32)
    logits = jax.random.normal(key_noise, full_shape, jnp.float32) * temper - decay_slope * distance
    logits = jnp.where(key_pos <= query_pos, logits, -1000000000.0)
    return jax.nn.softmax(logits, axis=-1).astype(jnp.bfloat16)


def draw_sequence_bounds(key, part):
    key_prompt, key_extra, key_pick = jax.random.split(key, 3)
    pair_index = jnp.arange(PAIRS, dtype=jnp.int32)
    prompt = jax.random.randint(key_prompt, (PAIRS,), 1, SEQ // 4 + 1, jnp.int32)
    base_length = SEQ // 8 + SEQ // 2 * pair_index // PAIRS
    extra = jax.random.randint(key_extra, (PAIRS, 2), 0, SEQ // 8 + 1, jnp.int32)
    ends = jnp.minimum(prompt[:, None] + base_length[:, None] + extra, SEQ)
    picked = jax.random.randint(key_pick, (), 0, PAIRS, jnp.int32)
    full_end = (pair_index == picked)[:, None] & (jnp.arange(2, dtype=jnp.int32)[None, :] == 1)
    ends = jnp.where(full_end, SEQ, ends)
    return jnp.concatenate([prompt[:, None], ends], axis=1).astype(jnp.int32)


def levels(stream_key, dims, shards, smallest, largest):
    def one(position, shards_of):
        steps = jax.random.uniform(jax.random.fold_in(jax.random.fold_in(stream_key, 6), position), (shards_of,), jnp.float32, smallest / len(shards), largest / len(shards))
        return jnp.repeat(jnp.exp(steps), dims[position] // shards_of).reshape((-1,) + (1,) * (len(dims) - position - 1))

    factor_of = one(*shards[0])
    for cut in shards[1:]:
        factor_of = factor_of * one(*cut)
    return factor_of


def gaussian(stream_key, dims, deviation, most, cuts=(), held_as=jnp.bfloat16):
    factor_of = levels(stream_key, dims, cuts, -0.22, 0.18) if cuts else 1.0
    drawn = jax.random.normal(stream_key, dims, jnp.float32) * deviation * factor_of
    return jnp.minimum(jnp.maximum(drawn, -most), most).astype(held_as)


def setup_inputs(seed: int = 0) -> dict:
    key_of = jax.random.split(jax.random.key(seed), 10)
    hidden_in = draw_hidden_in(jax.random.fold_in(key_of[9], 71), 0)
    attention_probs = draw_attention_probs(jax.random.fold_in(key_of[9], 71), 0)
    norm_gain = jnp.clip(1.0 + 0.1 * jax.random.normal(key_of[2], (N_PIPE, D), jnp.float32), 0.5, 1.5)
    value_weight = gaussian(key_of[3], (N_PIPE, D, KV_HEADS * HEAD_DIM), D ** -0.5, 0.09375, ((0, 2), (2, 2)))
    output_weight = gaussian(key_of[4], (N_PIPE, HEADS * HEAD_DIM, D), (HEADS * HEAD_DIM) ** -0.5, 0.125, ((0, 2), (1, 2)))
    head_grad = gaussian(key_of[5], (PAIRS, 2, SEQ, D), 4.0, 16.0, ((0, 8), (1, 2)))
    policy_logprob = jnp.clip(-3.0 + 2.8 * jax.random.uniform(key_of[6], (PAIRS, 2, SEQ), jnp.float32) ** levels(key_of[6], (PAIRS, 2, SEQ), ((0, 8),), -0.2, 0.2), -3.0, -0.2)
    reference_logprob = jnp.clip(-96.0 + 83.2 * jax.random.uniform(key_of[7], (PAIRS, 2), jnp.float32) ** levels(key_of[7], (PAIRS, 2), ((0, 8),), -0.2, 0.2), -96.0, -12.8)
    sequence_bounds = draw_sequence_bounds(jax.random.fold_in(key_of[9], 71), 0)
    return dict(hidden_in=hidden_in, attention_probs=attention_probs, norm_gain=norm_gain, value_weight=value_weight, output_weight=output_weight, head_grad=head_grad, policy_logprob=policy_logprob, reference_logprob=reference_logprob, sequence_bounds=sequence_bounds)


EPSILON = 1e-06
DPO_BETA = 0.25
LIKELIHOOD_COEF = 0.2

def section_backward(inputs, pattern, gain_vector, value_matrix, output_matrix, upstream):
    group_size = HEADS // KV_HEADS
    input_float = inputs.astype(jnp.float32)
    inverse_rms = lax.rsqrt(lax.optimization_barrier(jnp.mean(input_float * input_float, axis=-1, keepdims=True)) + EPSILON)
    normed = (input_float * inverse_rms * gain_vector).astype(jnp.bfloat16)
    values = jnp.einsum('pcsd,dk->pcsk', normed.astype(jnp.float32), value_matrix.astype(jnp.float32)).astype(jnp.bfloat16)
    grouped = pattern.astype(jnp.float32).reshape(PAIRS, 2, KV_HEADS, group_size, SEQ, SEQ)
    values_heads = values.astype(jnp.float32).reshape(PAIRS, 2, SEQ, KV_HEADS, HEAD_DIM)
    mixed = jnp.einsum('pckgst,pctke->pcskge', grouped, values_heads).astype(jnp.bfloat16)
    mixed = mixed.reshape(PAIRS, 2, SEQ, HEADS * HEAD_DIM)
    upstream_float = upstream.astype(jnp.float32)
    mixed_grad = jnp.einsum('pcsd,hd->pcsh', upstream_float, output_matrix.astype(jnp.float32)).astype(jnp.bfloat16)
    mixed_heads = mixed_grad.astype(jnp.float32).reshape(PAIRS, 2, SEQ, KV_HEADS, group_size, HEAD_DIM)
    values_grad = jnp.einsum('pckgst,pcskge->pctke', grouped, mixed_heads).astype(jnp.bfloat16)
    values_grad = values_grad.reshape(PAIRS, 2, SEQ, KV_HEADS * HEAD_DIM)
    group_columns = KV_HEADS * HEAD_DIM // N_TENSOR
    grad_groups = values_grad.astype(jnp.float32).reshape(PAIRS, 2, SEQ, N_TENSOR, group_columns)
    weight_groups = value_matrix.astype(jnp.float32).reshape(D, N_TENSOR, group_columns)
    normed_grad = jnp.zeros((PAIRS, 2, SEQ, D), jnp.float32)
    for group_index in range(N_TENSOR):
        group_term = jnp.einsum('pcsk,dk->pcsd', grad_groups[:, :, :, group_index, :], weight_groups[:, group_index, :])
        rounded = lax.optimization_barrier(group_term.astype(jnp.bfloat16))
        normed_grad = normed_grad + rounded.astype(jnp.float32)
    gain_total = lax.optimization_barrier(jnp.sum(normed_grad * input_float * inverse_rms, axis=(0, 1, 2)))
    scaled = normed_grad * gain_vector
    cubed = inverse_rms * inverse_rms * inverse_rms
    input_grad = inverse_rms * scaled - input_float * cubed * lax.optimization_barrier(jnp.mean(input_float * scaled, axis=-1, keepdims=True))
    new_rows = (upstream_float + input_grad).astype(jnp.bfloat16)
    mixed_total = jnp.einsum('pcsd,pcsh->dh', upstream_float, mixed.astype(jnp.float32))
    value_total = jnp.einsum('pcsd,pcsk->dk', normed.astype(jnp.float32), values_grad.astype(jnp.float32))
    return (new_rows, value_total, mixed_total, gain_total)

def reference(hidden_in, attention_probs, norm_gain, value_weight, output_weight, head_grad, policy_logprob, reference_logprob, sequence_bounds):
    positions = jnp.arange(SEQ, dtype=jnp.int32)
    response_bool = (positions[None, None, :] >= sequence_bounds[:, 0:1, None]) & (positions[None, None, :] < sequence_bounds[:, 1:3, None])
    response_mask = response_bool.astype(jnp.float32)
    sequence_logprob = lax.optimization_barrier(jnp.sum(response_mask * policy_logprob, axis=-1))
    margin = DPO_BETA * (sequence_logprob[:, 0] - reference_logprob[:, 0] - (sequence_logprob[:, 1] - reference_logprob[:, 1]))
    weight_pair = jax.nn.sigmoid(-margin)
    chosen_total = jnp.sum(response_bool[:, 0, :].astype(jnp.int32))
    likelihood_scale = LIKELIHOOD_COEF * jnp.asarray(PAIRS, jnp.float32) / chosen_total.astype(jnp.float32)
    chosen_weight = -DPO_BETA * weight_pair[:, None] * response_mask[:, 0] - likelihood_scale * response_mask[:, 0]
    rejected_weight = DPO_BETA * weight_pair[:, None] * response_mask[:, 1]
    token_weight = jnp.stack([chosen_weight, rejected_weight], axis=1)
    upstream = (token_weight[..., None] * head_grad.astype(jnp.float32)).astype(jnp.bfloat16)
    cotangents = []
    value_list = []
    output_list = []
    gain_list = []
    for section_index in range(N_PIPE - 1, -1, -1):
        upstream, value_total, mixed_total, gain_total = section_backward(hidden_in[section_index], attention_probs[section_index], norm_gain[section_index], value_weight[section_index], output_weight[section_index], upstream)
        cotangents.insert(0, upstream)
        value_list.insert(0, value_total)
        output_list.insert(0, mixed_total)
        gain_list.insert(0, gain_total)
    return (jnp.stack(cotangents), jnp.stack(value_list), jnp.stack(output_list), jnp.stack(gain_list))
```

```python
import functools

import jax
import jax.numpy as jnp
from jax import lax
from jax.experimental import pallas as pl
from jax.experimental.pallas import tpu as pltpu
from jax.sharding import PartitionSpec as P

LANES = 128
BAND = 16
MESH = pl.DeviceIdType.MESH

EPSILON = 1e-06
DPO_BETA = 0.25
LIKELIHOOD_COEF = 0.2


def greet(peers):
    barrier = pltpu.get_barrier_semaphore()
    total = 0
    for axis, n in peers:
        me = lax.axis_index(axis)

        @pl.loop(1, n)
        def _(k):
            pl.semaphore_signal(
                barrier, inc=1, device_id={axis: lax.rem(me + k, n)}, device_id_type=MESH
            )

        total += n - 1
    pl.semaphore_wait(barrier, total)


def remote(src, dst, send_sem, recv_sem, **device):
    return pltpu.make_async_remote_copy(
        src_ref=src,
        dst_ref=dst,
        send_sem=send_sem,
        recv_sem=recv_sem,
        device_id=device,
        device_id_type=MESH,
    )


def aligned(start, size, to=None):
    return pl.ds(pl.multiple_of(start, to or size), size)


def bands(sequences, length):
    todo = sorted(
        ((b + 1) * BAND, b, s) for b in range(length // BAND) for s in range(sequences)
    )
    groups = []
    for width, b, s in sorted(todo, key=lambda t: (-t[0], t[2])):
        for group in groups:
            start = sum(w for w, _, _ in group)
            if start + width <= LANES:
                group.append((width, b, s))
                break
        else:
            groups.append([(width, b, s)])
    return groups


def layer_kernel(
    sizes,
    hidden_hbm,
    probs_hbm,
    gain_hbm,
    wv_hbm,
    wo_hbm,
    head_hbm,
    policy_hbm,
    refer_hbm,
    bounds_hbm,
    cot_ref,
    value_ref,
    out_ref,
    gain_out_ref,
    hid,
    prob,
    gain,
    wvc,
    wo,
    head,
    head_in,
    policy,
    refer,
    bound,
    bound_in,
    wcol,
    normed,
    rms,
    pack,
    packs,
    dy,
    turned,
    mg,
    vgt,
    vgc,
    ng,
    rows_ref,
    vpart,
    near_in,
    near_sum,
    value_in,
    dy_in,
    mixed,
    gain_own,
    gx,
    gx_in,
    load_sem,
    h_load,
    p_load,
    b_send,
    b_recv,
    h_send,
    h_recv,
    w_send,
    w_recv,
    z_send,
    z_recv,
    y_send,
    y_recv,
    d_send,
    d_recv,
    o_send,
    o_recv,
    v_send,
    v_recv,
    c_send,
    c_recv,
    n_send,
    n_recv,
    s_send,
    s_recv,
    g_send,
    g_recv,
):
    n, nt, np_ = sizes
    me, ti, pi = lax.axis_index("dp"), lax.axis_index("tensor"), lax.axis_index("pipe")
    micro, both, length, width = hidden_hbm.shape
    own = head_hbm.shape[1]
    tokens = micro * both * length
    part = tokens // nt
    per_part = part // length
    columns = wo.shape[0]
    heads = columns // LANES
    wcols = wv_hbm.shape[1]
    value_heads = wcols // LANES
    per_value = heads // value_heads
    rows = width // n
    fast = 2 if n % 2 == 0 else 1
    slow = n // fast
    line, side = lax.div(me, fast), lax.rem(me, fast)
    partner = me + 1 - 2 * side
    last = pi == np_ - 1
    groups = bands(micro * both, length)
    group_rows = heads * BAND
    value_base = len(groups) * group_rows

    def load(src, dst, i):
        return pltpu.make_async_copy(src, dst, load_sem.at[i])

    mine = aligned(ti * wcols, wcols)
    small = [
        load(bounds_hbm, bound, 0),
        load(policy_hbm, policy, 1),
        load(refer_hbm, refer, 2),
        load(gain_hbm, gain, 3),
    ]
    wv_load = load(wv_hbm, wvc.at[:, mine], 4)
    wo_load = load(wo_hbm, wo, 5)
    hid_loads, prob_loads, head_loads = [], [], []
    for c in range(both):
        for p in range(micro):
            s = c * micro + p
            hid_loads.append(
                pltpu.make_async_copy(
                    hidden_hbm.at[p, c], hid.at[pl.ds(s * length, length)], h_load.at[s]
                )
            )
            prob_loads.append(
                pltpu.make_async_copy(probs_hbm.at[p, c], prob.at[s], p_load.at[s])
            )
    for o in range(own):
        for p in range(micro):
            head_loads.append(load(head_hbm.at[p, o], head.at[o * micro + p], 6 + o * micro + p))
    small[0].start()

    @pl.when(last)
    def _():
        for copy in head_loads:
            copy.start()

    for copy in hid_loads + small[1:]:
        copy.start()
    wv_load.start()
    for copy in prob_loads:
        copy.start()
    wo_load.start()
    small[0].wait()
    greet((("dp", n), ("tensor", nt), ("pipe", np_)))

    def bound_copy(k):
        return remote(bound, bound_in.at[k], b_send.at[k], b_recv.at[k], dp=lax.rem(me + k, n))

    def head_copy(k, j):
        return remote(
            head.at[j], head_in.at[k, j], h_send.at[k, j], h_recv.at[k, j],
            tensor=lax.rem(ti + k, nt),
        )

    def wv_copy(k):
        return remote(
            wvc.at[:, mine], wvc.at[:, mine], w_send.at[k], w_recv.at[k],
            tensor=lax.rem(ti + k, nt),
        )

    def vg_copy(k, half):
        block = vgc.at[aligned(half * part, part), mine]
        return remote(
            block, block, v_send.at[k, half], v_recv.at[k, half], tensor=lax.rem(ti + k, nt)
        )

    def z_copy(k):
        return remote(
            pack, packs.at[me], z_send.at[k], z_recv.at[k], dp=lax.rem(me + fast * k, n)
        )

    def y_copy(k):
        src = lax.rem(me - fast * k + n, n)
        block = pack if isinstance(k, int) and k == 0 else packs.at[src]
        return remote(block, packs.at[src], y_send.at[k], y_recv.at[k], dp=partner)

    def dy_copy(k):
        peer = lax.rem(me + k, n)
        at = aligned(ti * part, part)
        return remote(
            turned.at[aligned(peer * rows, rows, 8), at], dy_in.at[k, :, at],
            d_send.at[k], d_recv.at[k], dp=peer,
        )

    def onward(j, k, half):
        block = dy_in.at[k, :, aligned(half * part, part)]
        return remote(
            block, block, o_send.at[j, k], o_recv.at[j, k], tensor=lax.rem(ti + j, nt)
        )

    def down_copy(half):
        at = aligned(half * part, part)
        return remote(
            rows_ref.at[at], dy.at[at], c_send.at[half], c_recv.at[half],
            pipe=lax.rem(pi - 1 + np_, np_),
        )

    def near_copy(j):
        block = j * fast + fast - 1 - side
        return remote(
            vpart.at[aligned(block * rows, rows, 8)], near_in.at[j], n_send.at[j], n_recv.at[j],
            dp=partner,
        )

    def value_copy(k):
        return remote(
            near_sum.at[lax.rem(line + k, slow)], value_in.at[k], s_send.at[k], s_recv.at[k],
            dp=lax.rem(me + fast * k, n),
        )

    def gain_copy(k):
        return remote(gx, gx_in.at[k], g_send.at[k], g_recv.at[k], tensor=lax.rem(ti + k, nt))

    @pl.loop(1, n)
    def _(k):
        bound_copy(k).start()

    @pl.when(last)
    def _():
        for j in range(per_part):
            head_loads[j].wait()
            for k in range(1, nt):
                head_copy(k, j).start()

    wv_load.wait()

    @pl.when(last)
    def _():
        for k in range(1, nt):
            wv_copy(k).start()

    for copy in small[1:]:
        copy.wait()
    for copy in hid_loads:
        copy.wait()

    @pl.loop(0, tokens // BAND)
    def _(i):
        at = aligned(i * BAND, BAND)
        x = hid[at, :].astype(jnp.float32)
        inverse = lax.rsqrt(jnp.mean(x * x, axis=-1, keepdims=True) + EPSILON)
        rms[at, :] = inverse
        normed[at, :] = (x * inverse * gain[...]).astype(jnp.bfloat16)

    values = jnp.dot(normed[...], wvc[:, mine], preferred_element_type=jnp.float32).astype(
        jnp.bfloat16
    )
    for v in range(value_heads):
        pack[value_base + v * tokens : value_base + (v + 1) * tokens, :] = values[
            :, v * LANES : (v + 1) * LANES
        ]
    for copy in prob_loads:
        copy.wait()
    for i, group in enumerate(groups):
        for h in range(heads):
            row = h * length
            cells = [
                prob[s, row + b * BAND : row + (b + 1) * BAND, 0:w] for w, b, s in group
            ]
            spare = LANES - sum(w for w, _, _ in group)
            if spare:
                cells.append(jnp.zeros((BAND, spare), jnp.bfloat16))
            pack[i * group_rows + h * BAND : i * group_rows + (h + 1) * BAND, :] = (
                jnp.concatenate(cells, axis=1)
            )
    if fast > 1:
        y_copy(0).start()

    @pl.loop(1, slow)
    def _(k):
        z_copy(k).start()

    packs[me] = pack[...]

    total = jnp.zeros((1, 1), jnp.int32)

    def responses(b):
        spans = jnp.minimum(b[:, 1:2], length) - jnp.maximum(b[:, 0:1], 0)
        return jnp.sum(jnp.maximum(spans, 0), axis=0, keepdims=True)

    total = responses(bound[...])
    for k in range(1, n):
        bound_copy(k).wait_recv()
        total = total + responses(bound_in[k])
    likelihood = LIKELIHOOD_COEF * micro * n / total.astype(jnp.float32)
    along = lax.broadcasted_iota(jnp.int32, (1, length), 1)
    down = lax.broadcasted_iota(jnp.int32, (length, 1), 0)
    for p in range(micro):
        low = bound[p : p + 1, 0:1]
        scores = []
        for c in range(both):
            high = bound[p : p + 1, 1 + c : 2 + c]
            inside = jnp.where((along >= low) & (along < high), policy[p, c : c + 1, :], 0.0)
            scores.append(
                jnp.sum(inside, axis=-1, keepdims=True) - refer[p : p + 1, c : c + 1]
            )
        margin = DPO_BETA * (scores[0] - scores[1])
        pair = jax.nn.sigmoid(-margin)
        for c in range(both):
            high = bound[p : p + 1, 1 + c : 2 + c]
            weight = -DPO_BETA * pair - likelihood if c == 0 else DPO_BETA * pair
            inside = (down >= low) & (down < high)
            wcol[(c * micro + p) * length : (c * micro + p + 1) * length, :] = jnp.where(
                inside, jnp.broadcast_to(weight, (length, 1)), 0.0
            )

    def forward():
        @pl.loop(1, slow)
        def _(k):
            z_copy(k).wait_recv()
            if fast > 1:
                y_copy(k).start()

    if np_ > 1:

        @pl.when(jnp.logical_not(last))
        def _():
            forward()
            for k in range(1, nt):
                wv_copy(k).start()

    wo_load.wait()

    @pl.loop(0, nt)
    def _(i):
        half = lax.rem(ti - i + nt, nt)
        at = aligned(half * part, part)

        def upstream(block):
            @pl.loop(0, part // BAND)
            def _(r):
                to = aligned(half * part + r * BAND, BAND)
                dy[to, :] = (wcol[to, :] * block(r).astype(jnp.float32)).astype(jnp.bfloat16)

        per = length // BAND

        @pl.when(last & (i == 0))
        def _():
            upstream(lambda r: head[lax.div(r, per), aligned(lax.rem(r, per) * BAND, BAND), :])

        @pl.when(last & (i > 0))
        def _():
            for j in range(per_part):
                head_copy(i, j).wait_recv()
            upstream(
                lambda r: head_in[i, lax.div(r, per), aligned(lax.rem(r, per) * BAND, BAND), :]
            )

        if np_ > 1:

            @pl.when(jnp.logical_not(last))
            def _():
                down_copy(half).wait_recv()

        @pl.loop(0, width // LANES)
        def _(j):
            to = aligned(j * LANES, LANES)
            turned[to, at] = dy[at, to].T

        @pl.when(i == 0)
        def _():
            @pl.loop(1, n)
            def _(k):
                dy_copy(k).start()

        mg[...] = jnp.dot(wo[...], turned[:, at], preferred_element_type=jnp.float32).astype(
            jnp.bfloat16
        )
        for v in range(value_heads):
            across = []
            for j in range(per_part):
                stacked = jnp.concatenate(
                    [
                        mg[h * LANES : (h + 1) * LANES, j * length : (j + 1) * length]
                        for h in range(v * per_value, (v + 1) * per_value)
                    ],
                    axis=1,
                )
                pattern = prob[
                    half * per_part + j, v * per_value * length : (v + 1) * per_value * length, :
                ]
                across.append(jnp.dot(stacked, pattern, preferred_element_type=jnp.float32))
            block = jnp.concatenate(across, axis=1)
            vgt[v * LANES : (v + 1) * LANES, at] = block.astype(jnp.bfloat16)
            vgc[at, aligned(ti * wcols + v * LANES, LANES)] = block.T.astype(jnp.bfloat16)
        for k in range(1, nt):

            @pl.when((pi > 0) | (half == lax.rem(ti + k, nt)))
            def _():
                vg_copy(k, half).start()

    step = 2 * LANES if width % (2 * LANES) == 0 else LANES

    @pl.loop(0, width // step)
    def _(j):
        to = aligned(j * step, step)
        block = jnp.dot(vgt[...], normed[:, to], preferred_element_type=jnp.float32)
        vpart[to, :] = block.T.astype(jnp.bfloat16)

    if fast > 1:

        @pl.loop(0, slow)
        def _(j):
            near_copy(j).start()

    for k in range(1, nt):
        wv_copy(k).wait_recv()

    @pl.loop(0, nt)
    def _(i):
        half = lax.rem(ti + i, nt)
        at = aligned(half * part, part)

        @pl.when((i == 0) | (pi > 0))
        def _():
            for k in range(1, nt):
                vg_copy(k, half).wait_recv()
            ng[...] = lax.dot_general(
                vgc[at, :], wvc[...], (((1,), (1,)), ((), ())), preferred_element_type=jnp.float32
            )

            @pl.loop(0, part // BAND)
            def _(r):
                here = aligned(r * BAND, BAND)
                to = aligned(half * part + r * BAND, BAND)
                x = hid[to, :].astype(jnp.float32)
                inverse = rms[to, :]
                scaled = ng[here, :] * gain[...]
                mean = jnp.mean(x * scaled, axis=-1, keepdims=True)
                grad = inverse * scaled - x * (inverse * inverse * inverse * mean)
                rows_ref[to, :] = (dy[to, :].astype(jnp.float32) + grad).astype(jnp.bfloat16)

            if np_ > 1:

                @pl.when(pi > 0)
                def _():
                    down_copy(half).start()

    for o in range(own):
        for p in range(micro):
            cot_ref[p, o] = rows_ref[aligned(ti * part + (o * micro + p) * length, length), :]

    @pl.loop(0, slow)
    def _(j):
        near = vpart[aligned((j * fast + side) * rows, rows, 8), :].astype(jnp.float32)
        if fast > 1:
            near_copy(j).wait_recv()
            near = near + near_in[j].astype(jnp.float32)
        near_sum[j] = near.astype(jnp.bfloat16)

    @pl.loop(1, slow)
    def _(k):
        value_copy(k).start()

    @pl.when(last)
    def _():
        forward()

    if fast > 1:
        y_copy(0).wait_recv()

        @pl.loop(1, slow)
        def _(k):
            y_copy(k).wait_recv()

    def mix(src):
        for v in range(value_heads):
            for i, group in enumerate(groups):
                first = i * group_rows + v * per_value * BAND
                pattern = packs[src, first : first + per_value * BAND, :]
                blocks, start = [], 0
                for w, b, s in group:
                    key = value_base + v * tokens + s * length
                    cells = [packs[src, key : key + w, :]]
                    if start:
                        cells.insert(0, jnp.zeros((start, LANES), jnp.bfloat16))
                    if start + w < LANES:
                        cells.append(jnp.zeros((LANES - start - w, LANES), jnp.bfloat16))
                    blocks.append(jnp.concatenate(cells, axis=0) if len(cells) > 1 else cells[0])
                    start += w
                product = jnp.dot(
                    pattern,
                    jnp.concatenate(blocks, axis=1) if len(blocks) > 1 else blocks[0],
                    preferred_element_type=jnp.float32,
                ).astype(jnp.bfloat16)
                for j, (w, b, s) in enumerate(group):
                    row = s * length + b * BAND
                    for h in range(per_value):
                        column = (v * per_value + h) * LANES
                        mixed[row : row + BAND, column : column + LANES] = product[
                            h * BAND : (h + 1) * BAND, j * LANES : (j + 1) * LANES
                        ]

    mix(me)
    out_ref[...] = jnp.dot(
        turned[aligned(me * rows, rows, 8), :], mixed[...], preferred_element_type=jnp.float32
    )

    @pl.loop(1, n + 1)
    def _(k):
        @pl.when(k < n)
        def _():
            dy_copy(k).wait_recv()
            for j in range(1, nt):
                onward(j, k, ti).start()

        @pl.when(k > 1)
        def _():
            mix(lax.rem(me - k + 1 + n, n))
            for j in range(1, nt):
                onward(j, k - 1, lax.rem(ti - j + nt, nt)).wait_recv()
            out_ref[...] += jnp.dot(
                dy_in[k - 1], mixed[...], preferred_element_type=jnp.float32
            )

    for i in range(n):

        @pl.when(me == i)
        def _():
            gain_own[...] = gain[:, i * rows : (i + 1) * rows]

    value_ref[...] = near_sum[line].astype(jnp.float32)

    @pl.loop(1, slow)
    def _(k):
        value_copy(k).wait_recv()
        value_ref[...] += value_in[k].astype(jnp.float32)

    weighed = value_ref[...] * wvc[aligned(me * rows, rows, 8), mine].astype(jnp.float32)
    gx[...] = jnp.sum(weighed.T, axis=0, keepdims=True) / gain_own[...]
    for k in range(1, nt):
        gain_copy(k).start()
    gain_sum = gx[...]
    for k in range(1, nt):
        gain_copy(k).wait_recv()
        gain_sum = gain_sum + gx_in[k]
    gain_out_ref[...] = gain_sum

    @pl.loop(1, n)
    def _(k):
        bound_copy(k).wait_send()
        dy_copy(k).wait_send()
        for j in range(1, nt):
            onward(j, k, ti).wait_send()

    @pl.loop(1, slow)
    def _(k):
        z_copy(k).wait_send()
        value_copy(k).wait_send()
        if fast > 1:
            y_copy(k).wait_send()

    if fast > 1:
        y_copy(0).wait_send()

        @pl.loop(0, slow)
        def _(j):
            near_copy(j).wait_send()

    for k in range(1, nt):
        wv_copy(k).wait_send()
        gain_copy(k).wait_send()
        for half in range(nt):

            @pl.when((pi > 0) | (half == lax.rem(ti + k, nt)))
            def _():
                vg_copy(k, half).wait_send()

    @pl.when(last)
    def _():
        for k in range(1, nt):
            for j in range(per_part):
                head_copy(k, j).wait_send()

    if np_ > 1:

        @pl.when(pi > 0)
        def _():
            for half in range(nt):
                down_copy(half).wait_send()


def layer(sizes, hidden, probs, gain, wv, wo, head, policy, refer, bounds):
    n, nt, _ = sizes
    micro, both, length, width = hidden.shape
    own = head.shape[1]
    tokens = micro * both * length
    sequences = micro * both
    columns = wo.shape[0]
    heads = columns // LANES
    wcols = wv.shape[1]
    rows = width // n
    part = tokens // nt
    fast = 2 if n % 2 == 0 else 1
    slow = n // fast
    pack_rows = (
        len(bands(sequences, length)) * heads * BAND + wcols // LANES * tokens
    )
    vmem = pl.BlockSpec(memory_space=pltpu.VMEM)
    dma = pltpu.SemaphoreType.DMA
    bf, f32, i32 = jnp.bfloat16, jnp.float32, jnp.int32
    return pl.pallas_call(
        functools.partial(layer_kernel, sizes),
        out_shape=(
            jax.ShapeDtypeStruct((micro, own, length, width), bf),
            jax.ShapeDtypeStruct((rows, wcols), f32),
            jax.ShapeDtypeStruct((rows, columns), f32),
            jax.ShapeDtypeStruct((1, rows), f32),
        ),
        in_specs=[pl.BlockSpec(memory_space=pl.ANY)] * 9,
        out_specs=(vmem,) * 4,
        scratch_shapes=[
            pltpu.VMEM((tokens, width), bf),
            pltpu.VMEM((sequences, heads * length, length), bf),
            pltpu.VMEM((1, width), f32),
            pltpu.VMEM((width, nt * wcols), bf),
            pltpu.VMEM((columns, width), bf),
            pltpu.VMEM((own * micro, length, width), bf),
            pltpu.VMEM((nt, own * micro, length, width), bf),
            pltpu.VMEM(policy.shape, f32),
            pltpu.VMEM(refer.shape, f32),
            pltpu.VMEM(bounds.shape, i32),
            pltpu.VMEM((n,) + bounds.shape, i32),
            pltpu.VMEM((tokens, 1), f32),
            pltpu.VMEM((tokens, width), bf),
            pltpu.VMEM((tokens, 1), f32),
            pltpu.VMEM((pack_rows, LANES), bf),
            pltpu.VMEM((n, pack_rows, LANES), bf),
            pltpu.VMEM((tokens, width), bf),
            pltpu.VMEM((width, tokens), bf),
            pltpu.VMEM((columns, part), bf),
            pltpu.VMEM((wcols, tokens), bf),
            pltpu.VMEM((tokens, nt * wcols), bf),
            pltpu.VMEM((part, width), f32),
            pltpu.VMEM((tokens, width), bf),
            pltpu.VMEM((width, wcols), bf),
            pltpu.VMEM((slow, rows, wcols), bf),
            pltpu.VMEM((slow, rows, wcols), bf),
            pltpu.VMEM((slow, rows, wcols), bf),
            pltpu.VMEM((n, rows, tokens), bf),
            pltpu.VMEM((tokens, columns), bf),
            pltpu.VMEM((1, rows), f32),
            pltpu.VMEM((1, rows), f32),
            pltpu.VMEM((nt, 1, rows), f32),
            dma((6 + own * micro,)),
            dma((sequences,)),
            dma((sequences,)),
            dma((n,)),
            dma((n,)),
            dma((nt, own * micro)),
            dma((nt, own * micro)),
            dma((nt,)),
            dma((nt,)),
            dma((slow,)),
            dma((slow,)),
            dma((slow,)),
            dma((slow,)),
            dma((n,)),
            dma((n,)),
            dma((nt, n)),
            dma((nt, n)),
            dma((nt, nt)),
            dma((nt, nt)),
            dma((nt,)),
            dma((nt,)),
            dma((slow,)),
            dma((slow,)),
            dma((slow,)),
            dma((slow,)),
            dma((nt,)),
            dma((nt,)),
        ],
        compiler_params=pltpu.CompilerParams(
            collective_id=0, has_side_effects=True, vmem_limit_bytes=63 * 2**20
        ),
        name="layer",
    )(hidden, probs, gain, wv, wo, head, policy, refer, bounds)


def body(
    hidden_in,
    attention_probs,
    norm_gain,
    value_weight,
    output_weight,
    head_grad,
    policy_logprob,
    reference_logprob,
    sequence_bounds,
):
    sizes = tuple(lax.axis_size(a) for a in ("dp", "tensor", "pipe"))
    micro, both, heads, length, _ = attention_probs.shape[1:]
    cotangent, value, output, gain = layer(
        sizes,
        hidden_in[0],
        attention_probs[0].reshape(micro, both, heads * length, length),
        norm_gain,
        value_weight[0],
        output_weight[0],
        head_grad,
        policy_logprob,
        reference_logprob,
        sequence_bounds,
    )
    return (cotangent[None], value[None], output[None], gain)


def solution(mesh):
    in_specs = (
        P("pipe", "dp", None, None, None),
        P("pipe", "dp", None, "tensor", None, None),
        P("pipe", None),
        P("pipe", None, "tensor"),
        P("pipe", "tensor", None),
        P("dp", "tensor", None, None),
        P("dp", None, None),
        P("dp", None),
        P("dp", None),
    )
    out_specs = (
        P("pipe", "dp", "tensor", None, None),
        P("pipe", "dp", "tensor"),
        P("pipe", "dp", "tensor"),
        P("pipe", "dp"),
    )
    return jax.shard_map(body, mesh=mesh, in_specs=in_specs, out_specs=out_specs, check_vma=False)
```

```python
import functools

import jax
import jax.numpy as jnp
from jax import lax
from jax.experimental import pallas as pl
from jax.experimental.pallas import tpu as pltpu
from jax.sharding import PartitionSpec as P

LANES = 128
BAND = 16
MESH = pl.DeviceIdType.MESH

EPSILON = 1e-06
DPO_BETA = 0.25
LIKELIHOOD_COEF = 0.2


def greet(peers):
    barrier = pltpu.get_barrier_semaphore()
    total = 0
    for axis, n in peers:
        me = lax.axis_index(axis)

        @pl.loop(1, n)
        def _(k):
            pl.semaphore_signal(
                barrier, inc=1, device_id={axis: lax.rem(me + k, n)}, device_id_type=MESH
            )

        total += n - 1
    pl.semaphore_wait(barrier, total)


def remote(src, dst, send_sem, recv_sem, **device):
    return pltpu.make_async_remote_copy(
        src_ref=src,
        dst_ref=dst,
        send_sem=send_sem,
        recv_sem=recv_sem,
        device_id=device,
        device_id_type=MESH,
    )


def aligned(start, size, to=None):
    return pl.ds(pl.multiple_of(start, to or size), size)


def bands(sequences, length):
    todo = sorted(
        ((b + 1) * BAND, b, s) for b in range(length // BAND) for s in range(sequences)
    )
    groups = []
    for width, b, s in sorted(todo, key=lambda t: (-t[0], t[2])):
        for group in groups:
            start = sum(w for w, _, _ in group)
            if start + width <= LANES:
                group.append((width, b, s))
                break
        else:
            groups.append([(width, b, s)])
    return groups


def layer_kernel(
    sizes,
    hidden_hbm,
    probs_hbm,
    gain_hbm,
    wv_hbm,
    wo_hbm,
    head_hbm,
    policy_hbm,
    refer_hbm,
    bounds_hbm,
    cot_ref,
    value_ref,
    out_ref,
    gain_out_ref,
    hid,
    prob,
    gain,
    wvc,
    wo,
    head,
    head_in,
    policy,
    refer,
    bound,
    bound_in,
    wcol,
    normed,
    rms,
    packs,
    dy,
    turned,
    mg,
    vgt,
    vgc,
    ng,
    rows_ref,
    vpart,
    near_in,
    near_sum,
    value_in,
    dy_in,
    mixed,
    gain_own,
    gx,
    gx_in,
    load_sem,
    h_load,
    p_load,
    b_send,
    b_recv,
    h_send,
    h_recv,
    w_send,
    w_recv,
    r_send,
    r_recv,
    l_send,
    l_recv,
    y_send,
    y_recv,
    d_send,
    d_recv,
    o_send,
    o_recv,
    v_send,
    v_recv,
    c_send,
    c_recv,
    n_send,
    n_recv,
    s_send,
    s_recv,
    g_send,
    g_recv,
):
    n, nt, np_ = sizes
    me, ti, pi = lax.axis_index("dp"), lax.axis_index("tensor"), lax.axis_index("pipe")
    micro, both, length, width = hidden_hbm.shape
    own = head_hbm.shape[1]
    tokens = micro * both * length
    part = tokens // nt
    per_part = part // length
    columns = wo.shape[0]
    heads = columns // LANES
    wcols = wv_hbm.shape[1]
    value_heads = wcols // LANES
    per_value = heads // value_heads
    rows = width // n
    fast = 2 if n % 2 == 0 else 1
    slow = n // fast
    line, side = lax.div(me, fast), lax.rem(me, fast)
    partner = me + 1 - 2 * side
    last = pi == np_ - 1
    groups = bands(micro * both, length)
    group_rows = heads * BAND
    value_base = len(groups) * group_rows
    pack_parts = ((0, value_base), (value_base, tokens * value_heads))

    def load(src, dst, i):
        return pltpu.make_async_copy(src, dst, load_sem.at[i])

    mine = aligned(ti * wcols, wcols)
    small = [
        load(bounds_hbm, bound, 0),
        load(policy_hbm, policy, 1),
        load(refer_hbm, refer, 2),
        load(gain_hbm, gain, 3),
    ]
    wv_load = load(wv_hbm, wvc.at[:, mine], 4)
    wo_load = load(wo_hbm, wo, 5)
    hid_loads, prob_loads, head_loads = [], [], []
    for c in range(both):
        for p in range(micro):
            s = c * micro + p
            hid_loads.append(
                pltpu.make_async_copy(
                    hidden_hbm.at[p, c], hid.at[pl.ds(s * length, length)], h_load.at[s]
                )
            )
            prob_loads.append(
                pltpu.make_async_copy(probs_hbm.at[p, c], prob.at[s], p_load.at[s])
            )
    for o in range(own):
        for p in range(micro):
            head_loads.append(load(head_hbm.at[p, o], head.at[o * micro + p], 6 + o * micro + p))
    small[0].start()

    @pl.when(last)
    def _():
        for copy in head_loads:
            copy.start()

    for copy in hid_loads + small[1:]:
        copy.start()
    wv_load.start()
    for copy in prob_loads:
        copy.start()
    wo_load.start()
    small[0].wait()
    greet((("dp", n), ("tensor", nt), ("pipe", np_)))

    def bound_copy(k):
        return remote(bound, bound_in.at[k], b_send.at[k], b_recv.at[k], dp=lax.rem(me + k, n))

    def head_copy(k, j):
        return remote(
            head.at[j], head_in.at[k, j], h_send.at[k, j], h_recv.at[k, j],
            tensor=lax.rem(ti + k, nt),
        )

    def wv_copy(k):
        return remote(
            wvc.at[:, mine], wvc.at[:, mine], w_send.at[k], w_recv.at[k],
            tensor=lax.rem(ti + k, nt),
        )

    def vg_copy(k, half):
        block = vgc.at[aligned(half * part, part), mine]
        return remote(
            block, block, v_send.at[k, half], v_recv.at[k, half], tensor=lax.rem(ti + k, nt)
        )

    def pack_copy(q, b, send, recv, peer):
        block = packs.at[b * fast + side, pl.ds(*pack_parts[q])]
        return remote(block, block, send.at[q, b], recv.at[q, b], dp=peer)

    def right_copy(q, b):
        return pack_copy(q, b, r_send, r_recv, lax.rem(me + fast, n))

    def left_copy(q, b):
        return pack_copy(q, b, l_send, l_recv, lax.rem(me - fast + n, n))

    def y_copy(q, b):
        return pack_copy(q, b, y_send, y_recv, partner)

    def send_pack(q, b):
        @pl.when((line < slow - 1) & (b <= line))
        def _():
            right_copy(q, b).start()

        @pl.when((line > 0) & (b >= line))
        def _():
            left_copy(q, b).start()

        if fast > 1:
            y_copy(q, b).start()

    def relay(low, high):
        @pl.loop(low, high)
        def _(d):
            for q in range(2):

                @pl.when(line >= d)
                def _():
                    right_copy(q, line - d).wait_recv()
                    send_pack(q, line - d)

                @pl.when(line + d < slow)
                def _():
                    left_copy(q, line + d).wait_recv()
                    send_pack(q, line + d)

    def dy_copy(k):
        peer = lax.rem(me + k, n)
        at = aligned(ti * part, part)
        return remote(
            turned.at[aligned(peer * rows, rows, 8), at], dy_in.at[k, :, at],
            d_send.at[k], d_recv.at[k], dp=peer,
        )

    def onward(j, k, half):
        block = dy_in.at[k, :, aligned(half * part, part)]
        return remote(
            block, block, o_send.at[j, k], o_recv.at[j, k], tensor=lax.rem(ti + j, nt)
        )

    def down_copy(half):
        at = aligned(half * part, part)
        return remote(
            rows_ref.at[at], dy.at[at], c_send.at[half], c_recv.at[half],
            pipe=lax.rem(pi - 1 + np_, np_),
        )

    def near_copy(j):
        block = j * fast + fast - 1 - side
        return remote(
            vpart.at[aligned(block * rows, rows, 8)], near_in.at[j], n_send.at[j], n_recv.at[j],
            dp=partner,
        )

    def value_copy(k):
        return remote(
            near_sum.at[lax.rem(line + k, slow)], value_in.at[k], s_send.at[k], s_recv.at[k],
            dp=lax.rem(me + fast * k, n),
        )

    def gain_copy(k):
        return remote(gx, gx_in.at[k], g_send.at[k], g_recv.at[k], tensor=lax.rem(ti + k, nt))

    @pl.loop(1, n)
    def _(k):
        bound_copy(k).start()

    @pl.when(last)
    def _():
        for j in range(per_part):
            head_loads[j].wait()
            for k in range(1, nt):
                head_copy(k, j).start()

    wv_load.wait()

    @pl.when(last)
    def _():
        for k in range(1, nt):
            wv_copy(k).start()

    for copy in prob_loads:
        copy.wait()
    for i, group in enumerate(groups):
        for h in range(heads):
            row = h * length
            cells = [
                prob[s, row + b * BAND : row + (b + 1) * BAND, 0:w] for w, b, s in group
            ]
            spare = LANES - sum(w for w, _, _ in group)
            if spare:
                cells.append(jnp.zeros((BAND, spare), jnp.bfloat16))
            first = i * group_rows + h * BAND
            packs[me, first : first + BAND, :] = jnp.concatenate(cells, axis=1)
    send_pack(0, line)

    def responses(b):
        spans = jnp.minimum(b[:, 1:2], length) - jnp.maximum(b[:, 0:1], 0)
        return jnp.sum(jnp.maximum(spans, 0), axis=0, keepdims=True)

    for copy in small[1:]:
        copy.wait()
    total = responses(bound[...])
    for k in range(1, n):
        bound_copy(k).wait_recv()
        total = total + responses(bound_in[k])
    likelihood = LIKELIHOOD_COEF * micro * n / total.astype(jnp.float32)
    along = lax.broadcasted_iota(jnp.int32, (1, length), 1)
    down = lax.broadcasted_iota(jnp.int32, (length, 1), 0)
    for p in range(micro):
        low = bound[p : p + 1, 0:1]
        scores = []
        for c in range(both):
            high = bound[p : p + 1, 1 + c : 2 + c]
            inside = jnp.where((along >= low) & (along < high), policy[p, c : c + 1, :], 0.0)
            scores.append(
                jnp.sum(inside, axis=-1, keepdims=True) - refer[p : p + 1, c : c + 1]
            )
        margin = DPO_BETA * (scores[0] - scores[1])
        pair = jax.nn.sigmoid(-margin)
        for c in range(both):
            high = bound[p : p + 1, 1 + c : 2 + c]
            weight = -DPO_BETA * pair - likelihood if c == 0 else DPO_BETA * pair
            inside = (down >= low) & (down < high)
            wcol[(c * micro + p) * length : (c * micro + p + 1) * length, :] = jnp.where(
                inside, jnp.broadcast_to(weight, (length, 1)), 0.0
            )

    def half_of(half):
        return aligned(half * part, part)

    def upstream(half, block):
        per = length // BAND

        @pl.loop(0, part // BAND)
        def _(r):
            to = aligned(half * part + r * BAND, BAND)
            rows_in = block(lax.div(r, per), aligned(lax.rem(r, per) * BAND, BAND))
            dy[to, :] = (wcol[to, :] * rows_in.astype(jnp.float32)).astype(jnp.bfloat16)

    lots = next(c for c in (4, 2, 1) if width // LANES % c == 0)

    def turn(half):
        at = half_of(half)

        @pl.loop(0, width // (LANES * lots))
        def _(j):
            for i in range(lots):
                to = aligned((j * lots + i) * LANES, LANES)
                turned[to, at] = dy[at, to].T

    def send_dy():
        @pl.loop(1, n)
        def _(k):
            dy_copy(k).start()

    def values_grad(half):
        at = half_of(half)
        for v in range(value_heads):
            across = []
            for j in range(per_part):
                stacked = jnp.concatenate(
                    [
                        mg[h * LANES : (h + 1) * LANES, at][:, j * length : (j + 1) * length]
                        for h in range(v * per_value, (v + 1) * per_value)
                    ],
                    axis=1,
                )
                pattern = prob[
                    half * per_part + j, v * per_value * length : (v + 1) * per_value * length, :
                ]
                across.append(jnp.dot(stacked, pattern, preferred_element_type=jnp.float32))
            block = jnp.concatenate(across, axis=1)
            vgt[v * LANES : (v + 1) * LANES, at] = block.astype(jnp.bfloat16)
            vgc[at, aligned(ti * wcols + v * LANES, LANES)] = block.T.astype(jnp.bfloat16)
        for k in range(1, nt):

            @pl.when((pi > 0) | (half == lax.rem(ti + k, nt)))
            def _():
                vg_copy(k, half).start()

    def mixed_grad(at):
        mg[:, at] = jnp.dot(
            wo[...], turned[:, at], preferred_element_type=jnp.float32
        ).astype(jnp.bfloat16)

    def norm_backward():
        for k in range(1, nt):
            wv_copy(k).wait_recv()

        @pl.loop(0, nt)
        def _(i):
            half = lax.rem(ti + i, nt)

            @pl.when((i == 0) | (pi > 0))
            def _():
                for k in range(1, nt):
                    vg_copy(k, half).wait_recv()
                ng[...] = lax.dot_general(
                    vgc[half_of(half), :],
                    wvc[...],
                    (((1,), (1,)), ((), ())),
                    preferred_element_type=jnp.float32,
                )

                @pl.loop(0, part // BAND)
                def _(r):
                    here = aligned(r * BAND, BAND)
                    to = aligned(half * part + r * BAND, BAND)
                    x = hid[to, :].astype(jnp.float32)
                    inverse = rms[to, :]
                    scaled = ng[here, :] * gain[...]
                    mean = jnp.mean(x * scaled, axis=-1, keepdims=True)
                    grad = inverse * scaled - x * (inverse * inverse * inverse * mean)
                    rows_ref[to, :] = (dy[to, :].astype(jnp.float32) + grad).astype(jnp.bfloat16)

                if np_ > 1:

                    @pl.when(pi > 0)
                    def _():
                        down_copy(half).start()


        for o in range(own):
            for p in range(micro):
                cot_ref[p, o] = rows_ref[aligned(ti * part + (o * micro + p) * length, length), :]

    def pass_on(low, high):
        @pl.loop(low, high)
        def _(k):
            dy_copy(k).wait_recv()
            for j in range(1, nt):
                onward(j, k, ti).start()

    @pl.when(last)
    def _():
        upstream(ti, lambda s, at: head[s, at, :])
        turn(ti)
        send_dy()

    for copy in hid_loads:
        copy.wait()

    @pl.loop(0, tokens // BAND)
    def _(i):
        at = aligned(i * BAND, BAND)
        x = hid[at, :].astype(jnp.float32)
        inverse = lax.rsqrt(jnp.mean(x * x, axis=-1, keepdims=True) + EPSILON)
        rms[at, :] = inverse
        normed[at, :] = (x * inverse * gain[...]).astype(jnp.bfloat16)

    values = jnp.dot(normed[...], wvc[:, mine], preferred_element_type=jnp.float32).astype(
        jnp.bfloat16
    )
    for v in range(value_heads):
        packs[me, value_base + v * tokens : value_base + (v + 1) * tokens, :] = values[
            :, v * LANES : (v + 1) * LANES
        ]
    send_pack(1, line)
    wo_load.wait()

    @pl.when(last)
    def _():
        mixed_grad(half_of(ti))
        values_grad(ti)
        for i in range(1, nt):
            half = lax.rem(ti - i + nt, nt)
            for j in range(per_part):
                head_copy(i, j).wait_recv()
            upstream(half, lambda s, at: head_in[i, s, at, :])
            turn(half)
            mixed_grad(half_of(half))
            values_grad(half)
        relay(1, min(2, slow))
        norm_backward()
        pass_on(1, n)

    early = min(3, n)
    middle = min(5, n)

    if np_ > 1:

        @pl.when(jnp.logical_not(last))
        def _():
            relay(1, slow)
            for i in range(nt):
                half = lax.rem(ti + i, nt)
                down_copy(half).wait_recv()
                turn(half)
                if i == 0:
                    send_dy()
                    for k in range(1, nt):
                        wv_copy(k).start()
            mixed_grad(slice(None))
            for i in range(nt):
                values_grad(lax.rem(ti - 1 - i + 2 * nt, nt))

    for v in range(value_heads):
        ng[0:LANES, :] = jnp.dot(
            vgt[v * LANES : (v + 1) * LANES, :], normed[...], preferred_element_type=jnp.float32
        )

        @pl.loop(0, width // (LANES * lots))
        def _(j):
            for i in range(lots):
                to = aligned((j * lots + i) * LANES, LANES)
                vpart[to, v * LANES : (v + 1) * LANES] = (
                    ng[0:LANES, to].astype(jnp.bfloat16).T
                )

    if fast > 1:

        @pl.loop(0, slow)
        def _(j):
            near_copy(j).start()

    @pl.when(last)
    def _():
        relay(min(2, slow), slow)

    if np_ > 1:

        @pl.when(jnp.logical_not(last))
        def _():
            pass_on(1, early)

    @pl.loop(0, slow)
    def _(j):
        near = vpart[aligned((j * fast + side) * rows, rows, 8), :].astype(jnp.float32)
        if fast > 1:
            near_copy(j).wait_recv()
            near = near + near_in[j].astype(jnp.float32)
        near_sum[j] = near.astype(jnp.bfloat16)

    @pl.loop(1, slow)
    def _(k):
        value_copy(k).start()

    if np_ > 1:

        @pl.when(jnp.logical_not(last))
        def _():
            pass_on(early, middle)

    if fast > 1:

        @pl.loop(0, slow)
        def _(b):
            y_copy(0, b).wait_recv()
            y_copy(1, b).wait_recv()

    def mix(src):
        for v in range(value_heads):
            for i, group in enumerate(groups):
                first = i * group_rows + v * per_value * BAND
                pattern = packs[src, first : first + per_value * BAND, :]
                blocks, start = [], 0
                for w, b, s in group:
                    key = value_base + v * tokens + s * length
                    cells = [packs[src, key : key + w, :]]
                    if start:
                        cells.insert(0, jnp.zeros((start, LANES), jnp.bfloat16))
                    if start + w < LANES:
                        cells.append(jnp.zeros((LANES - start - w, LANES), jnp.bfloat16))
                    blocks.append(jnp.concatenate(cells, axis=0) if len(cells) > 1 else cells[0])
                    start += w
                product = jnp.dot(
                    pattern,
                    jnp.concatenate(blocks, axis=1) if len(blocks) > 1 else blocks[0],
                    preferred_element_type=jnp.float32,
                ).astype(jnp.bfloat16)
                for j, (w, b, s) in enumerate(group):
                    row = s * length + b * BAND
                    for h in range(per_value):
                        column = (v * per_value + h) * LANES
                        mixed[row : row + BAND, column : column + LANES] = product[
                            h * BAND : (h + 1) * BAND, j * LANES : (j + 1) * LANES
                        ]

    mix(me)
    out_ref[...] = jnp.dot(
        turned[aligned(me * rows, rows, 8), :], mixed[...], preferred_element_type=jnp.float32
    )

    if np_ > 1:

        @pl.when(jnp.logical_not(last))
        def _():
            norm_backward()

    lag = 2

    @pl.loop(1, n + lag)
    def _(k):
        if np_ > 1:

            @pl.when(jnp.logical_not(last) & (k >= middle) & (k < n))
            def _():
                dy_copy(k).wait_recv()
                for j in range(1, nt):
                    onward(j, k, ti).start()

        @pl.when(k > lag)
        def _():
            mix(lax.rem(me - k + lag + n, n))
            for j in range(1, nt):
                onward(j, k - lag, lax.rem(ti - j + nt, nt)).wait_recv()
            out_ref[...] += jnp.dot(
                dy_in[k - lag], mixed[...], preferred_element_type=jnp.float32
            )

    for i in range(n):

        @pl.when(me == i)
        def _():
            gain_own[...] = gain[:, i * rows : (i + 1) * rows]

    value_ref[...] = near_sum[line].astype(jnp.float32)

    @pl.loop(1, slow)
    def _(k):
        value_copy(k).wait_recv()
        value_ref[...] += value_in[k].astype(jnp.float32)

    weighed = value_ref[...] * wvc[aligned(me * rows, rows, 8), mine].astype(jnp.float32)
    gx[...] = jnp.sum(weighed.T, axis=0, keepdims=True) / gain_own[...]
    for k in range(1, nt):
        gain_copy(k).start()
    gain_sum = gx[...]
    for k in range(1, nt):
        gain_copy(k).wait_recv()
        gain_sum = gain_sum + gx_in[k]
    gain_out_ref[...] = gain_sum

    @pl.loop(1, n)
    def _(k):
        bound_copy(k).wait_send()
        dy_copy(k).wait_send()
        for j in range(1, nt):
            onward(j, k, ti).wait_send()

    @pl.loop(1, slow)
    def _(k):
        value_copy(k).wait_send()

    @pl.loop(0, slow)
    def _(b):
        for q in range(2):

            @pl.when((line < slow - 1) & (b <= line))
            def _():
                right_copy(q, b).wait_send()

            @pl.when((line > 0) & (b >= line))
            def _():
                left_copy(q, b).wait_send()

            if fast > 1:
                y_copy(q, b).wait_send()
        if fast > 1:
            near_copy(b).wait_send()

    for k in range(1, nt):
        wv_copy(k).wait_send()
        gain_copy(k).wait_send()
        for half in range(nt):

            @pl.when((pi > 0) | (half == lax.rem(ti + k, nt)))
            def _():
                vg_copy(k, half).wait_send()

    @pl.when(last)
    def _():
        for k in range(1, nt):
            for j in range(per_part):
                head_copy(k, j).wait_send()

    if np_ > 1:

        @pl.when(pi > 0)
        def _():
            for half in range(nt):
                down_copy(half).wait_send()


def layer(sizes, hidden, probs, gain, wv, wo, head, policy, refer, bounds):
    n, nt, _ = sizes
    micro, both, length, width = hidden.shape
    own = head.shape[1]
    tokens = micro * both * length
    sequences = micro * both
    columns = wo.shape[0]
    heads = columns // LANES
    wcols = wv.shape[1]
    rows = width // n
    part = tokens // nt
    fast = 2 if n % 2 == 0 else 1
    slow = n // fast
    pack_rows = (
        len(bands(sequences, length)) * heads * BAND + wcols // LANES * tokens
    )
    vmem = pl.BlockSpec(memory_space=pltpu.VMEM)
    dma = pltpu.SemaphoreType.DMA
    bf, f32, i32 = jnp.bfloat16, jnp.float32, jnp.int32
    return pl.pallas_call(
        functools.partial(layer_kernel, sizes),
        out_shape=(
            jax.ShapeDtypeStruct((micro, own, length, width), bf),
            jax.ShapeDtypeStruct((rows, wcols), f32),
            jax.ShapeDtypeStruct((rows, columns), f32),
            jax.ShapeDtypeStruct((1, rows), f32),
        ),
        in_specs=[pl.BlockSpec(memory_space=pl.ANY)] * 9,
        out_specs=(vmem,) * 4,
        scratch_shapes=[
            pltpu.VMEM((tokens, width), bf),
            pltpu.VMEM((sequences, heads * length, length), bf),
            pltpu.VMEM((1, width), f32),
            pltpu.VMEM((width, nt * wcols), bf),
            pltpu.VMEM((columns, width), bf),
            pltpu.VMEM((own * micro, length, width), bf),
            pltpu.VMEM((nt, own * micro, length, width), bf),
            pltpu.VMEM(policy.shape, f32),
            pltpu.VMEM(refer.shape, f32),
            pltpu.VMEM(bounds.shape, i32),
            pltpu.VMEM((n,) + bounds.shape, i32),
            pltpu.VMEM((tokens, 1), f32),
            pltpu.VMEM((tokens, width), bf),
            pltpu.VMEM((tokens, 1), f32),
            pltpu.VMEM((n, pack_rows, LANES), bf),
            pltpu.VMEM((tokens, width), bf),
            pltpu.VMEM((width, tokens), bf),
            pltpu.VMEM((columns, tokens), bf),
            pltpu.VMEM((wcols, tokens), bf),
            pltpu.VMEM((tokens, nt * wcols), bf),
            pltpu.VMEM((part, width), f32),
            pltpu.VMEM((tokens, width), bf),
            pltpu.VMEM((width, wcols), bf),
            pltpu.VMEM((slow, rows, wcols), bf),
            pltpu.VMEM((slow, rows, wcols), bf),
            pltpu.VMEM((slow, rows, wcols), bf),
            pltpu.VMEM((n, rows, tokens), bf),
            pltpu.VMEM((tokens, columns), bf),
            pltpu.VMEM((1, rows), f32),
            pltpu.VMEM((1, rows), f32),
            pltpu.VMEM((nt, 1, rows), f32),
            dma((6 + own * micro,)),
            dma((sequences,)),
            dma((sequences,)),
            dma((n,)),
            dma((n,)),
            dma((nt, own * micro)),
            dma((nt, own * micro)),
            dma((nt,)),
            dma((nt,)),
            dma((2, slow)),
            dma((2, slow)),
            dma((2, slow)),
            dma((2, slow)),
            dma((2, slow)),
            dma((2, slow)),
            dma((n,)),
            dma((n,)),
            dma((nt, n)),
            dma((nt, n)),
            dma((nt, nt)),
            dma((nt, nt)),
            dma((nt,)),
            dma((nt,)),
            dma((slow,)),
            dma((slow,)),
            dma((slow,)),
            dma((slow,)),
            dma((nt,)),
            dma((nt,)),
        ],
        compiler_params=pltpu.CompilerParams(
            collective_id=0, has_side_effects=True, vmem_limit_bytes=63 * 2**20
        ),
        name="layer",
    )(hidden, probs, gain, wv, wo, head, policy, refer, bounds)


def body(
    hidden_in,
    attention_probs,
    norm_gain,
    value_weight,
    output_weight,
    head_grad,
    policy_logprob,
    reference_logprob,
    sequence_bounds,
):
    sizes = tuple(lax.axis_size(a) for a in ("dp", "tensor", "pipe"))
    micro, both, heads, length, _ = attention_probs.shape[1:]
    cotangent, value, output, gain = layer(
        sizes,
        hidden_in[0],
        attention_probs[0].reshape(micro, both, heads * length, length),
        norm_gain,
        value_weight[0],
        output_weight[0],
        head_grad,
        policy_logprob,
        reference_logprob,
        sequence_bounds,
    )
    return (cotangent[None], value[None], output[None], gain)


def solution(mesh):
    in_specs = (
        P("pipe", "dp", None, None, None),
        P("pipe", "dp", None, "tensor", None, None),
        P("pipe", None),
        P("pipe", None, "tensor"),
        P("pipe", "tensor", None),
        P("dp", "tensor", None, None),
        P("dp", None, None),
        P("dp", None),
        P("dp", None),
    )
    out_specs = (
        P("pipe", "dp", "tensor", None, None),
        P("pipe", "dp", "tensor"),
        P("pipe", "dp", "tensor"),
        P("pipe", "dp"),
    )
    return jax.shard_map(body, mesh=mesh, in_specs=in_specs, out_specs=out_specs, check_vma=False)
```

```python
import functools

import jax
import jax.numpy as jnp
from jax import lax
from jax.experimental import pallas as pl
from jax.experimental.pallas import tpu as pltpu
from jax.sharding import PartitionSpec as P

LANES = 128
BAND = 16
MESH = pl.DeviceIdType.MESH

EPSILON = 1e-06
DPO_BETA = 0.25
LIKELIHOOD_COEF = 0.2


def greet(peers):
    barrier = pltpu.get_barrier_semaphore()
    total = 0
    for axis, n in peers:
        me = lax.axis_index(axis)

        @pl.loop(1, n)
        def _(k):
            pl.semaphore_signal(
                barrier, inc=1, device_id={axis: lax.rem(me + k, n)}, device_id_type=MESH
            )

        total += n - 1
    pl.semaphore_wait(barrier, total)


def remote(src, dst, send_sem, recv_sem, **device):
    return pltpu.make_async_remote_copy(
        src_ref=src,
        dst_ref=dst,
        send_sem=send_sem,
        recv_sem=recv_sem,
        device_id=device,
        device_id_type=MESH,
    )


def aligned(start, size, to=None):
    return pl.ds(pl.multiple_of(start, to or size), size)


def bands(sequences, length):
    todo = sorted(
        ((b + 1) * BAND, b, s) for b in range(length // BAND) for s in range(sequences)
    )
    groups = []
    for width, b, s in sorted(todo, key=lambda t: (-t[0], t[2])):
        for group in groups:
            start = sum(w for w, _, _ in group)
            if start + width <= LANES:
                group.append((width, b, s))
                break
        else:
            groups.append([(width, b, s)])
    return groups


def layer_kernel(
    sizes,
    hidden_hbm,
    probs_hbm,
    gain_hbm,
    wv_hbm,
    wo_hbm,
    head_hbm,
    policy_hbm,
    refer_hbm,
    bounds_hbm,
    cot_ref,
    value_ref,
    out_ref,
    gain_out_ref,
    hid,
    prob,
    gain,
    wvc,
    wo,
    head,
    head_in,
    policy,
    refer,
    bound,
    bound_in,
    wcol,
    normed,
    rms,
    packs,
    dy,
    turned,
    mg,
    mg_half,
    vgt,
    vgc,
    ng,
    rows_ref,
    vpart,
    near_in,
    near_sum,
    value_in,
    dy_in,
    mixed,
    gain_own,
    gx,
    gx_in,
    load_sem,
    h_load,
    p_load,
    b_send,
    b_recv,
    h_send,
    h_recv,
    w_send,
    w_recv,
    r_send,
    r_recv,
    l_send,
    l_recv,
    y_send,
    y_recv,
    d_send,
    d_recv,
    o_send,
    o_recv,
    v_send,
    v_recv,
    c_send,
    c_recv,
    n_send,
    n_recv,
    s_send,
    s_recv,
    g_send,
    g_recv,
):
    n, nt, np_ = sizes
    me, ti, pi = lax.axis_index("dp"), lax.axis_index("tensor"), lax.axis_index("pipe")
    micro, both, length, width = hidden_hbm.shape
    own = head_hbm.shape[1]
    tokens = micro * both * length
    part = tokens // nt
    per_part = part // length
    columns = wo.shape[0]
    heads = columns // LANES
    wcols = wv_hbm.shape[1]
    value_heads = wcols // LANES
    per_value = heads // value_heads
    rows = width // n
    fast = 2 if n % 2 == 0 else 1
    slow = n // fast
    line, side = lax.div(me, fast), lax.rem(me, fast)
    partner = me + 1 - 2 * side
    last = pi == np_ - 1
    groups = bands(micro * both, length)
    group_rows = heads * BAND
    value_base = len(groups) * group_rows
    pack_parts = ((0, value_base), (value_base, tokens * value_heads))

    def load(src, dst, i):
        return pltpu.make_async_copy(src, dst, load_sem.at[i])

    mine = aligned(ti * wcols, wcols)
    small = [
        load(bounds_hbm, bound, 0),
        load(policy_hbm, policy, 1),
        load(refer_hbm, refer, 2),
        load(gain_hbm, gain, 3),
    ]
    wv_load = load(wv_hbm, wvc.at[:, mine], 4)
    wo_load = load(wo_hbm, wo, 5)
    hid_loads, prob_loads, head_loads = [], [], []
    for c in range(both):
        for p in range(micro):
            s = c * micro + p
            hid_loads.append(
                pltpu.make_async_copy(
                    hidden_hbm.at[p, c], hid.at[pl.ds(s * length, length)], h_load.at[s]
                )
            )
            prob_loads.append(
                pltpu.make_async_copy(probs_hbm.at[p, c], prob.at[s], p_load.at[s])
            )
    for o in range(own):
        for p in range(micro):
            head_loads.append(load(head_hbm.at[p, o], head.at[o * micro + p], 6 + o * micro + p))
    small[0].start()

    @pl.when(last)
    def _():
        for copy in head_loads:
            copy.start()

    for copy in hid_loads + small[1:]:
        copy.start()
    wv_load.start()
    for copy in prob_loads:
        copy.start()
    wo_load.start()
    greet((("dp", n), ("tensor", nt), ("pipe", np_)))

    def bound_copy(k):
        return remote(bound, bound_in.at[k], b_send.at[k], b_recv.at[k], dp=lax.rem(me + k, n))

    def head_copy(k, j):
        return remote(
            head.at[j], head_in.at[k, j], h_send.at[k, j], h_recv.at[k, j],
            tensor=lax.rem(ti + k, nt),
        )

    def wv_copy(k):
        return remote(
            wvc.at[:, mine], wvc.at[:, mine], w_send.at[k], w_recv.at[k],
            tensor=lax.rem(ti + k, nt),
        )

    def vg_copy(k, half):
        block = vgc.at[aligned(half * part, part), mine]
        return remote(
            block, block, v_send.at[k, half], v_recv.at[k, half], tensor=lax.rem(ti + k, nt)
        )

    def pack_copy(q, b, send, recv, peer):
        block = packs.at[b * fast + side, pl.ds(*pack_parts[q])]
        return remote(block, block, send.at[q, b], recv.at[q, b], dp=peer)

    def right_copy(q, b):
        return pack_copy(q, b, r_send, r_recv, lax.rem(me + fast, n))

    def left_copy(q, b):
        return pack_copy(q, b, l_send, l_recv, lax.rem(me - fast + n, n))

    def y_copy(q, b):
        return pack_copy(q, b, y_send, y_recv, partner)

    def send_pack(q, b):
        @pl.when((line < slow - 1) & (b <= line))
        def _():
            right_copy(q, b).start()

        @pl.when((line > 0) & (b >= line))
        def _():
            left_copy(q, b).start()

        if fast > 1:
            y_copy(q, b).start()

    def relay(parts, low, high):
        @pl.loop(low, high)
        def _(d):
            for q in parts:

                @pl.when(line >= d)
                def _():
                    right_copy(q, line - d).wait_recv()
                    send_pack(q, line - d)

                @pl.when(line + d < slow)
                def _():
                    left_copy(q, line + d).wait_recv()
                    send_pack(q, line + d)

    def dy_copy(k):
        peer = lax.rem(me + k, n)
        at = aligned(ti * part, part)
        return remote(
            turned.at[aligned(peer * rows, rows, 8), at], dy_in.at[k, :, at],
            d_send.at[k], d_recv.at[k], dp=peer,
        )

    def onward(j, k, half):
        block = dy_in.at[k, :, aligned(half * part, part)]
        return remote(
            block, block, o_send.at[j, k], o_recv.at[j, k], tensor=lax.rem(ti + j, nt)
        )

    def down_copy(half):
        at = aligned(half * part, part)
        return remote(
            rows_ref.at[at], dy.at[at], c_send.at[half], c_recv.at[half],
            pipe=lax.rem(pi - 1 + np_, np_),
        )

    def near_copy(j):
        block = j * fast + fast - 1 - side
        return remote(
            vpart.at[aligned(block * rows, rows, 8)], near_in.at[j], n_send.at[j], n_recv.at[j],
            dp=partner,
        )

    def value_copy(k):
        return remote(
            near_sum.at[lax.rem(line + k, slow)], value_in.at[k], s_send.at[k], s_recv.at[k],
            dp=lax.rem(me + fast * k, n),
        )

    def gain_copy(k):
        return remote(gx, gx_in.at[k], g_send.at[k], g_recv.at[k], tensor=lax.rem(ti + k, nt))

    small[0].wait()

    @pl.loop(1, n)
    def _(k):
        bound_copy(k).start()

    @pl.when(last)
    def _():
        for j in range(per_part):
            head_loads[j].wait()
            for k in range(1, nt):
                head_copy(k, j).start()

    wv_load.wait()

    @pl.when(last)
    def _():
        for k in range(1, nt):
            wv_copy(k).start()

    for copy in prob_loads:
        copy.wait()
    for i, group in enumerate(groups):
        for h in range(heads):
            row = h * length
            cells = [
                prob[s, row + b * BAND : row + (b + 1) * BAND, 0:w] for w, b, s in group
            ]
            spare = LANES - sum(w for w, _, _ in group)
            if spare:
                cells.append(jnp.zeros((BAND, spare), jnp.bfloat16))
            first = i * group_rows + h * BAND
            packs[me, first : first + BAND, :] = jnp.concatenate(cells, axis=1)
    send_pack(0, line)

    def half_of(half):
        return aligned(half * part, part)

    def upstream(half, block):
        per = length // BAND

        @pl.loop(0, part // BAND)
        def _(r):
            to = aligned(half * part + r * BAND, BAND)
            rows_in = block(lax.div(r, per), aligned(lax.rem(r, per) * BAND, BAND))
            dy[to, :] = (wcol[to, :] * rows_in.astype(jnp.float32)).astype(jnp.bfloat16)

    lots = next(c for c in (4, 2, 1) if width // LANES % c == 0)

    def turn(half):
        at = half_of(half)

        @pl.loop(0, width // (LANES * lots))
        def _(j):
            for i in range(lots):
                to = aligned((j * lots + i) * LANES, LANES)
                turned[to, at] = dy[at, to].T

    def send_dy():
        @pl.loop(1, n)
        def _(k):
            dy_copy(k).start()

    def values_grad(half, source, base):
        at = half_of(half)
        for v in range(value_heads):
            across = []
            for j in range(per_part):
                stacked = jnp.concatenate(
                    [
                        source[
                            h * LANES : (h + 1) * LANES,
                            base + j * length : base + (j + 1) * length,
                        ]
                        for h in range(v * per_value, (v + 1) * per_value)
                    ],
                    axis=1,
                )
                pattern = prob[
                    half * per_part + j, v * per_value * length : (v + 1) * per_value * length, :
                ]
                across.append(jnp.dot(stacked, pattern, preferred_element_type=jnp.float32))
            block = jnp.concatenate(across, axis=1)
            vgt[v * LANES : (v + 1) * LANES, at] = block.astype(jnp.bfloat16)
            vgc[at, aligned(ti * wcols + v * LANES, LANES)] = block.T.astype(jnp.bfloat16)
        for k in range(1, nt):

            @pl.when((pi > 0) | (half == lax.rem(ti + k, nt)))
            def _():
                vg_copy(k, half).start()

    def mixed_grad(half):
        if half is None:
            mg[...] = jnp.dot(wo[...], turned[...], preferred_element_type=jnp.float32).astype(
                jnp.bfloat16
            )
        else:
            mg_half[...] = jnp.dot(
                wo[...], turned[:, half_of(half)], preferred_element_type=jnp.float32
            ).astype(jnp.bfloat16)

    def norm_backward():
        for k in range(1, nt):
            wv_copy(k).wait_recv()

        @pl.loop(0, nt)
        def _(i):
            half = lax.rem(ti + i, nt)

            @pl.when((i == 0) | (pi > 0))
            def _():
                for k in range(1, nt):
                    vg_copy(k, half).wait_recv()
                ng[...] = lax.dot_general(
                    vgc[half_of(half), :],
                    wvc[...],
                    (((1,), (1,)), ((), ())),
                    preferred_element_type=jnp.float32,
                )

                @pl.loop(0, part // BAND)
                def _(r):
                    here = aligned(r * BAND, BAND)
                    to = aligned(half * part + r * BAND, BAND)
                    x = hid[to, :].astype(jnp.float32)
                    inverse = rms[to, :]
                    scaled = ng[here, :] * gain[...]
                    mean = jnp.mean(x * scaled, axis=-1, keepdims=True)
                    grad = inverse * scaled - x * (inverse * inverse * inverse * mean)
                    rows_ref[to, :] = (dy[to, :].astype(jnp.float32) + grad).astype(jnp.bfloat16)

                if np_ > 1:

                    @pl.when(pi > 0)
                    def _():
                        down_copy(half).start()


        for o in range(own):
            for p in range(micro):
                cot_ref[p, o] = rows_ref[aligned(ti * part + (o * micro + p) * length, length), :]

    def pass_on(low, high):
        @pl.loop(low, high)
        def _(k):
            dy_copy(k).wait_recv()
            for j in range(1, nt):
                onward(j, k, ti).start()

    for copy in small[1:]:
        copy.wait()
    for copy in hid_loads:
        copy.wait()

    @pl.loop(0, tokens // BAND)
    def _(i):
        at = aligned(i * BAND, BAND)
        x = hid[at, :].astype(jnp.float32)
        inverse = lax.rsqrt(jnp.mean(x * x, axis=-1, keepdims=True) + EPSILON)
        rms[at, :] = inverse
        normed[at, :] = (x * inverse * gain[...]).astype(jnp.bfloat16)

    values = jnp.dot(normed[...], wvc[:, mine], preferred_element_type=jnp.float32).astype(
        jnp.bfloat16
    )
    for v in range(value_heads):
        packs[me, value_base + v * tokens : value_base + (v + 1) * tokens, :] = values[
            :, v * LANES : (v + 1) * LANES
        ]
    send_pack(1, line)
    wo_load.wait()

    def responses(b):
        spans = jnp.minimum(b[:, 1:2], length) - jnp.maximum(b[:, 0:1], 0)
        return jnp.sum(jnp.maximum(spans, 0), axis=0, keepdims=True)

    total = responses(bound[...])
    for k in range(1, n):
        bound_copy(k).wait_recv()
        total = total + responses(bound_in[k])
    likelihood = LIKELIHOOD_COEF * micro * n / total.astype(jnp.float32)
    along = lax.broadcasted_iota(jnp.int32, (1, length), 1)
    down = lax.broadcasted_iota(jnp.int32, (length, 1), 0)
    for p in range(micro):
        low = bound[p : p + 1, 0:1]
        scores = []
        for c in range(both):
            high = bound[p : p + 1, 1 + c : 2 + c]
            inside = jnp.where((along >= low) & (along < high), policy[p, c : c + 1, :], 0.0)
            scores.append(
                jnp.sum(inside, axis=-1, keepdims=True) - refer[p : p + 1, c : c + 1]
            )
        margin = DPO_BETA * (scores[0] - scores[1])
        pair = jax.nn.sigmoid(-margin)
        for c in range(both):
            high = bound[p : p + 1, 1 + c : 2 + c]
            weight = -DPO_BETA * pair - likelihood if c == 0 else DPO_BETA * pair
            inside = (down >= low) & (down < high)
            wcol[(c * micro + p) * length : (c * micro + p + 1) * length, :] = jnp.where(
                inside, jnp.broadcast_to(weight, (length, 1)), 0.0
            )

    def mix(src):
        for v in range(value_heads):
            for i, group in enumerate(groups):
                first = i * group_rows + v * per_value * BAND
                pattern = packs[src, first : first + per_value * BAND, :]
                blocks, start = [], 0
                for w, b, s in group:
                    key = value_base + v * tokens + s * length
                    cells = [packs[src, key : key + w, :]]
                    if start:
                        cells.insert(0, jnp.zeros((start, LANES), jnp.bfloat16))
                    if start + w < LANES:
                        cells.append(jnp.zeros((LANES - start - w, LANES), jnp.bfloat16))
                    blocks.append(jnp.concatenate(cells, axis=0) if len(cells) > 1 else cells[0])
                    start += w
                product = jnp.dot(
                    pattern,
                    jnp.concatenate(blocks, axis=1) if len(blocks) > 1 else blocks[0],
                    preferred_element_type=jnp.float32,
                ).astype(jnp.bfloat16)
                for j, (w, b, s) in enumerate(group):
                    row = s * length + b * BAND
                    for h in range(per_value):
                        column = (v * per_value + h) * LANES
                        mixed[row : row + BAND, column : column + LANES] = product[
                            h * BAND : (h + 1) * BAND, j * LANES : (j + 1) * LANES
                        ]

    def value_part():
        for v in range(value_heads):
            ng[0:LANES, :] = jnp.dot(
                vgt[v * LANES : (v + 1) * LANES, :],
                normed[...],
                preferred_element_type=jnp.float32,
            )

            @pl.loop(0, width // (LANES * lots))
            def _(j):
                for i in range(lots):
                    to = aligned((j * lots + i) * LANES, LANES)
                    vpart[to, v * LANES : (v + 1) * LANES] = (
                        ng[0:LANES, to].astype(jnp.bfloat16).T
                    )

        if fast > 1:

            @pl.loop(0, slow)
            def _(j):
                near_copy(j).start()

    def near_sums():
        @pl.loop(0, slow)
        def _(j):
            near = vpart[aligned((j * fast + side) * rows, rows, 8), :].astype(jnp.float32)
            if fast > 1:
                near_copy(j).wait_recv()
                near = near + near_in[j].astype(jnp.float32)
            near_sum[j] = near.astype(jnp.bfloat16)

        @pl.loop(1, slow)
        def _(k):
            value_copy(k).start()

    def pack_waits():
        if fast > 1:

            @pl.loop(0, slow)
            def _(b):
                y_copy(0, b).wait_recv()
                y_copy(1, b).wait_recv()

    def own_product():
        mix(me)
        out_ref[...] = jnp.dot(
            turned[aligned(me * rows, rows, 8), :], mixed[...], preferred_element_type=jnp.float32
        )

    def products(low, high):
        @pl.loop(low, high)
        def _(k):
            mix(lax.rem(me - k + n, n))
            for j in range(1, nt):
                onward(j, k, lax.rem(ti - j + nt, nt)).wait_recv()
            out_ref[...] += jnp.dot(dy_in[k], mixed[...], preferred_element_type=jnp.float32)

    def value_final():
        for i in range(n):

            @pl.when(me == i)
            def _():
                gain_own[...] = gain[:, i * rows : (i + 1) * rows]

        value_ref[...] = near_sum[line].astype(jnp.float32)

        @pl.loop(1, slow)
        def _(k):
            value_copy(k).wait_recv()
            value_ref[...] += value_in[k].astype(jnp.float32)

        weighed = value_ref[...] * wvc[aligned(me * rows, rows, 8), mine].astype(jnp.float32)
        gx[...] = jnp.sum(weighed.T, axis=0, keepdims=True) / gain_own[...]
        for k in range(1, nt):
            gain_copy(k).start()

    @pl.when(last)
    def _():
        upstream(ti, lambda s, at: head[s, at, :])
        turn(ti)
        send_dy()
        mixed_grad(ti)
        values_grad(ti, mg_half, 0)
        relay((0, 1), 1, min(2, slow))
        for i in range(1, nt):
            half = lax.rem(ti - i + nt, nt)
            for j in range(per_part):
                head_copy(i, j).wait_recv()
            upstream(half, lambda s, at: head_in[i, s, at, :])
            turn(half)
            mixed_grad(half)
            values_grad(half, mg_half, 0)
        value_part()
        relay((0, 1), min(2, slow), min(3, slow))
        pass_on(1, n)
        norm_backward()
        relay((0, 1), min(3, slow), slow)
        near_sums()
        pack_waits()
        own_product()
        products(1, n)
        value_final()

    if np_ > 1:

        @pl.when(jnp.logical_not(last))
        def _():
            relay((0, 1), 1, slow)
            for i in range(nt):
                half = lax.rem(ti + i, nt)
                down_copy(half).wait_recv()
                turn(half)
                if i == 0:
                    send_dy()
                    for k in range(1, nt):
                        wv_copy(k).start()
            mixed_grad(None)
            for i in range(nt):
                values_grad(i, mg, i * part)
            value_part()
            pass_on(1, min(4, n))
            own_product()
            pass_on(min(4, n), n)
            pack_waits()
            near_sums()
            products(1, min(4, n))
            norm_backward()
            value_final()
            products(min(4, n), n)

    gain_sum = gx[...]
    for k in range(1, nt):
        gain_copy(k).wait_recv()
        gain_sum = gain_sum + gx_in[k]
    gain_out_ref[...] = gain_sum

    @pl.loop(1, n)
    def _(k):
        bound_copy(k).wait_send()
        dy_copy(k).wait_send()
        for j in range(1, nt):
            onward(j, k, ti).wait_send()

    @pl.loop(1, slow)
    def _(k):
        value_copy(k).wait_send()

    @pl.loop(0, slow)
    def _(b):
        for q in range(2):

            @pl.when((line < slow - 1) & (b <= line))
            def _():
                right_copy(q, b).wait_send()

            @pl.when((line > 0) & (b >= line))
            def _():
                left_copy(q, b).wait_send()

            if fast > 1:
                y_copy(q, b).wait_send()
        if fast > 1:
            near_copy(b).wait_send()

    for k in range(1, nt):
        wv_copy(k).wait_send()
        gain_copy(k).wait_send()
        for half in range(nt):

            @pl.when((pi > 0) | (half == lax.rem(ti + k, nt)))
            def _():
                vg_copy(k, half).wait_send()

    @pl.when(last)
    def _():
        for k in range(1, nt):
            for j in range(per_part):
                head_copy(k, j).wait_send()

    if np_ > 1:

        @pl.when(pi > 0)
        def _():
            for half in range(nt):
                down_copy(half).wait_send()


def layer(sizes, hidden, probs, gain, wv, wo, head, policy, refer, bounds):
    n, nt, _ = sizes
    micro, both, length, width = hidden.shape
    own = head.shape[1]
    tokens = micro * both * length
    sequences = micro * both
    columns = wo.shape[0]
    heads = columns // LANES
    wcols = wv.shape[1]
    rows = width // n
    part = tokens // nt
    fast = 2 if n % 2 == 0 else 1
    slow = n // fast
    pack_rows = (
        len(bands(sequences, length)) * heads * BAND + wcols // LANES * tokens
    )
    vmem = pl.BlockSpec(memory_space=pltpu.VMEM)
    dma = pltpu.SemaphoreType.DMA
    bf, f32, i32 = jnp.bfloat16, jnp.float32, jnp.int32
    return pl.pallas_call(
        functools.partial(layer_kernel, sizes),
        out_shape=(
            pltpu.VMEM((micro, own, length, width), bf),
            pltpu.VMEM((rows, wcols), f32),
            pltpu.VMEM((rows, columns), f32),
            pltpu.VMEM((1, rows), f32),
        ),
        in_specs=[pl.BlockSpec(memory_space=pl.ANY)] * 9,
        out_specs=(vmem,) * 4,
        scratch_shapes=[
            pltpu.VMEM((tokens, width), bf),
            pltpu.VMEM((sequences, heads * length, length), bf),
            pltpu.VMEM((1, width), f32),
            pltpu.VMEM((width, nt * wcols), bf),
            pltpu.VMEM((columns, width), bf),
            pltpu.VMEM((own * micro, length, width), bf),
            pltpu.VMEM((nt, own * micro, length, width), bf),
            pltpu.VMEM(policy.shape, f32),
            pltpu.VMEM(refer.shape, f32),
            pltpu.VMEM(bounds.shape, i32),
            pltpu.VMEM((n,) + bounds.shape, i32),
            pltpu.VMEM((tokens, 1), f32),
            pltpu.VMEM((tokens, width), bf),
            pltpu.VMEM((tokens, 1), f32),
            pltpu.VMEM((n, pack_rows, LANES), bf),
            pltpu.VMEM((tokens, width), bf),
            pltpu.VMEM((width, tokens), bf),
            pltpu.VMEM((columns, tokens), bf),
            pltpu.VMEM((columns, part), bf),
            pltpu.VMEM((wcols, tokens), bf),
            pltpu.VMEM((tokens, nt * wcols), bf),
            pltpu.VMEM((part, width), f32),
            pltpu.VMEM((tokens, width), bf),
            pltpu.VMEM((width, wcols), bf),
            pltpu.VMEM((slow, rows, wcols), bf),
            pltpu.VMEM((slow, rows, wcols), bf),
            pltpu.VMEM((slow, rows, wcols), bf),
            pltpu.VMEM((n, rows, tokens), bf),
            pltpu.VMEM((tokens, columns), bf),
            pltpu.VMEM((1, rows), f32),
            pltpu.VMEM((1, rows), f32),
            pltpu.VMEM((nt, 1, rows), f32),
            dma((6 + own * micro,)),
            dma((sequences,)),
            dma((sequences,)),
            dma((n,)),
            dma((n,)),
            dma((nt, own * micro)),
            dma((nt, own * micro)),
            dma((nt,)),
            dma((nt,)),
            dma((2, slow)),
            dma((2, slow)),
            dma((2, slow)),
            dma((2, slow)),
            dma((2, slow)),
            dma((2, slow)),
            dma((n,)),
            dma((n,)),
            dma((nt, n)),
            dma((nt, n)),
            dma((nt, nt)),
            dma((nt, nt)),
            dma((nt,)),
            dma((nt,)),
            dma((slow,)),
            dma((slow,)),
            dma((slow,)),
            dma((slow,)),
            dma((nt,)),
            dma((nt,)),
        ],
        compiler_params=pltpu.CompilerParams(
            collective_id=0, has_side_effects=True, vmem_limit_bytes=52 * 2**20
        ),
        name="layer",
    )(hidden, probs, gain, wv, wo, head, policy, refer, bounds)


def body(
    hidden_in,
    attention_probs,
    norm_gain,
    value_weight,
    output_weight,
    head_grad,
    policy_logprob,
    reference_logprob,
    sequence_bounds,
):
    sizes = tuple(lax.axis_size(a) for a in ("dp", "tensor", "pipe"))
    micro, both, heads, length, _ = attention_probs.shape[1:]
    cotangent, value, output, gain = layer(
        sizes,
        hidden_in[0],
        attention_probs[0].reshape(micro, both, heads * length, length),
        norm_gain,
        value_weight[0],
        output_weight[0],
        head_grad,
        policy_logprob,
        reference_logprob,
        sequence_bounds,
    )
    return (cotangent[None], value[None], output[None], gain)


def solution(mesh):
    in_specs = (
        P("pipe", "dp", None, None, None),
        P("pipe", "dp", None, "tensor", None, None),
        P("pipe", None),
        P("pipe", None, "tensor"),
        P("pipe", "tensor", None),
        P("dp", "tensor", None, None),
        P("dp", None, None),
        P("dp", None),
        P("dp", None),
    )
    out_specs = (
        P("pipe", "dp", "tensor", None, None),
        P("pipe", "dp", "tensor"),
        P("pipe", "dp", "tensor"),
        P("pipe", "dp"),
    )
    return jax.shard_map(body, mesh=mesh, in_specs=in_specs, out_specs=out_specs, check_vma=False)
```

```python
import functools

import jax
import jax.numpy as jnp
from jax import lax
from jax.experimental import pallas as pl
from jax.experimental.pallas import tpu as pltpu
from jax.sharding import PartitionSpec as P

LANES = 128
BAND = 16
MESH = pl.DeviceIdType.MESH

EPSILON = 1e-06
DPO_BETA = 0.25
LIKELIHOOD_COEF = 0.2


def greet(peers):
    barrier = pltpu.get_barrier_semaphore()
    total = 0
    for axis, n in peers:
        me = lax.axis_index(axis)

        @pl.loop(1, n)
        def _(k):
            pl.semaphore_signal(
                barrier, inc=1, device_id={axis: lax.rem(me + k, n)}, device_id_type=MESH
            )

        total += n - 1
    pl.semaphore_wait(barrier, total)


def remote(src, dst, send_sem, recv_sem, **device):
    return pltpu.make_async_remote_copy(
        src_ref=src,
        dst_ref=dst,
        send_sem=send_sem,
        recv_sem=recv_sem,
        device_id=device,
        device_id_type=MESH,
    )


def aligned(start, size, to=None):
    return pl.ds(pl.multiple_of(start, to or size), size)


def bands(sequences, length):
    todo = sorted(
        ((b + 1) * BAND, b, s) for b in range(length // BAND) for s in range(sequences)
    )
    groups = []
    for width, b, s in sorted(todo, key=lambda t: (-t[0], t[2])):
        for group in groups:
            start = sum(w for w, _, _ in group)
            if start + width <= LANES:
                group.append((width, b, s))
                break
        else:
            groups.append([(width, b, s)])
    return groups


def layer_kernel(
    sizes,
    hidden_hbm,
    probs_hbm,
    gain_hbm,
    wv_hbm,
    wo_hbm,
    head_hbm,
    policy_hbm,
    refer_hbm,
    bounds_hbm,
    cot_ref,
    value_ref,
    out_ref,
    gain_out_ref,
    hid,
    prob,
    gain,
    wvc,
    wo,
    head,
    head_in,
    policy,
    refer,
    bound,
    bound_in,
    wcol,
    normed,
    rms,
    packs,
    dy,
    turned,
    mg,
    mg_half,
    vgt,
    vgc,
    ng,
    rows_ref,
    vpart,
    near_in,
    near_sum,
    value_in,
    dy_in,
    mixed,
    wvt,
    gt,
    gt_in,
    gx,
    gx_in,
    load_sem,
    h_load,
    p_load,
    b_send,
    b_recv,
    h_send,
    h_recv,
    w_send,
    w_recv,
    a_send,
    a_recv,
    r_send,
    l_send,
    z_recv,
    y_send,
    y_recv,
    d_send,
    d_recv,
    o_send,
    o_recv,
    v_send,
    v_recv,
    c_send,
    c_recv,
    n_send,
    n_recv,
    s_send,
    s_recv,
    g_send,
    g_recv,
    t_send,
    t_recv,
    go,
):
    n, nt, np_ = sizes
    me, ti, pi = lax.axis_index("dp"), lax.axis_index("tensor"), lax.axis_index("pipe")
    micro, both, length, width = hidden_hbm.shape
    own = head_hbm.shape[1]
    tokens = micro * both * length
    part = tokens // nt
    per_part = part // length
    columns = wo.shape[0]
    heads = columns // LANES
    wcols = wv_hbm.shape[1]
    value_heads = wcols // LANES
    per_value = heads // value_heads
    rows = width // n
    fast = 2 if n % 2 == 0 else 1
    slow = n // fast
    line, side = lax.div(me, fast), lax.rem(me, fast)
    partner = me + 1 - 2 * side
    last = pi == np_ - 1
    groups = bands(micro * both, length)
    group_rows = heads * BAND
    value_base = len(groups) * group_rows
    pack_parts = ((0, value_base), (value_base, tokens * value_heads))

    def load(src, dst, i):
        return pltpu.make_async_copy(src, dst, load_sem.at[i])

    mine = aligned(ti * wcols, wcols)
    small = [
        load(bounds_hbm, bound, 0),
        load(policy_hbm, policy, 1),
        load(refer_hbm, refer, 2),
        load(gain_hbm, gain, 3),
    ]
    wv_load = load(wv_hbm, wvc.at[:, mine], 4)
    wo_load = load(wo_hbm, wo, 5)
    hid_loads, prob_loads, head_loads = [], [], []
    for c in range(both):
        for p in range(micro):
            s = c * micro + p
            hid_loads.append(
                pltpu.make_async_copy(
                    hidden_hbm.at[p, c], hid.at[pl.ds(s * length, length)], h_load.at[0]
                )
            )
            prob_loads.append(
                pltpu.make_async_copy(probs_hbm.at[p, c], prob.at[s], p_load.at[0])
            )
    for o in range(own):
        for p in range(micro):
            head_loads.append(load(head_hbm.at[p, o], head.at[o * micro + p], 6 + o * micro + p))
    small[0].start()

    @pl.when(last)
    def _():
        for copy in head_loads:
            copy.start()

    for copy in hid_loads + small[1:]:
        copy.start()
    wv_load.start()
    for copy in prob_loads:
        copy.start()
    wo_load.start()
    greet((("dp", n), ("tensor", nt), ("pipe", np_)))

    def both_ends(block, send, recv):
        return remote(block, block, send, recv, dp=lax.rem(me + 1, n))

    def bound_copy(k):
        return remote(bound, bound_in.at[k], b_send.at[0], b_recv.at[0], dp=lax.rem(me + k, n))

    bound_all = both_ends(bound_in.at[pl.ds(1, n - 1)], b_send.at[0], b_recv.at[0])

    def head_copy(k, j):
        return remote(
            head.at[j], head_in.at[k, j], h_send.at[k - 1, j], h_recv.at[k - 1, j],
            tensor=lax.rem(ti + k, nt),
        )

    quarter = width // 4

    def wv_copy(k, piece):
        block = wvc.at[aligned(piece * quarter, quarter, BAND), mine]
        return remote(
            block, block, w_send.at[k - 1, 1], w_recv.at[k - 1, 1], tensor=lax.rem(ti + k, nt)
        )

    def wv_other(k):
        return wvc.at[pl.ds(0, width // 2), aligned(lax.rem(ti - k + nt, nt) * wcols, wcols)]

    def wv_whole(k):
        block = wvc.at[:, mine]
        return remote(
            block, block, w_send.at[k - 1, 0], w_recv.at[k - 1, 0], tensor=lax.rem(ti + k, nt)
        )

    def wv_across(k, piece):
        at = aligned(lax.rem(ti - k + nt, nt) * wcols, wcols)
        block = wvc.at[aligned(piece * quarter, quarter, BAND), at]
        return remote(block, block, a_send.at[k - 1], a_recv.at[k - 1], dp=partner)

    def wv_half(k):
        return remote(
            wv_other(k), wv_other(k), w_send.at[k - 1, 1], w_recv.at[k - 1, 1],
            tensor=lax.rem(ti + k, nt),
        )

    pieces = (side, 2 + side)

    def wv_start(direct):
        for k in range(1, nt):
            if direct or fast == 1:
                wv_whole(k).start()
            else:
                for piece in pieces:
                    wv_copy(k, piece).start()

    def wv_arrive(direct):
        for k in range(1, nt):
            if direct or fast == 1:
                wv_whole(k).wait_recv()
            else:
                wv_half(k).wait_recv()
                for piece in pieces:
                    wv_across(k, piece).start()

    def wv_across_all(k):
        return both_ends(wv_other(k), a_send.at[k - 1], a_recv.at[k - 1])

    def wv_wait():
        if fast > 1:
            for k in range(1, nt):
                wv_across_all(k).wait_recv()

    def wv_sent(direct):
        for k in range(1, nt):
            if direct or fast == 1:
                wv_whole(k).wait_send()
            else:
                wv_half(k).wait_send()
                wv_across_all(k).wait_send()

    def go_on():
        if np_ > 1:

            @pl.when(pi > 0)
            def _():
                pl.semaphore_signal(go, inc=1, device_id={"pipe": pi - 1}, device_id_type=MESH)

    def vg_copy(k, half):
        block = vgc.at[aligned(half * part, part), mine]
        return remote(
            block, block, v_send.at[k - 1, half], v_recv.at[k - 1, half], tensor=lax.rem(ti + k, nt)
        )

    def pack_copy(q, b, send, peer):
        block = packs.at[b * fast + side, pl.ds(*pack_parts[q])]
        return remote(block, block, send.at[q, b], z_recv.at[q, b], dp=peer)

    def right_copy(q, b):
        return pack_copy(q, b, r_send, lax.rem(me + fast, n))

    def left_copy(q, b):
        return pack_copy(q, b, l_send, lax.rem(me - fast + n, n))

    def y_copy(q, b):
        block = packs.at[b * fast + side, pl.ds(*pack_parts[q])]
        return remote(block, block, y_send.at[0], y_recv.at[0], dp=partner)

    y_all = both_ends(packs.at[pl.ds(0, slow)], y_send.at[0], y_recv.at[0])

    def send_pack(q, b):
        @pl.when((line < slow - 1) & (b <= line))
        def _():
            right_copy(q, b).start()

        @pl.when((line > 0) & (b >= line))
        def _():
            left_copy(q, b).start()

        if fast > 1:
            y_copy(q, b).start()

    def relay(parts, low, high):
        @pl.loop(low, high)
        def _(d):
            for q in parts:

                @pl.when(line >= d)
                def _():
                    right_copy(q, line - d).wait_recv()
                    send_pack(q, line - d)

                @pl.when(line + d < slow)
                def _():
                    left_copy(q, line + d).wait_recv()
                    send_pack(q, line + d)

    def ahead(e):
        d, f = lax.div(e, fast), lax.rem(e, fast)
        there = lax.rem(line + d, slow) * fast + lax.rem(side + f, fast)
        back = lax.rem(line - d + slow, slow) * fast + lax.rem(side - f + fast, fast)
        return there, back

    def dy_copy(e):
        peer = ahead(e)[0]
        return remote(
            turned.at[aligned(peer * rows, rows, 8), aligned(ti * part, part)],
            dy_in.at[:, aligned(me * tokens + ti * part, part)],
            d_send.at[0], d_recv.at[e - 1], dp=peer,
        )

    def onward(j, e, half):
        block = dy_in.at[:, aligned(ahead(e)[1] * tokens + half * part, part)]
        return remote(
            block, block, o_send.at[j - 1], o_recv.at[j - 1, e - 1], tensor=lax.rem(ti + j, nt)
        )

    def down_copy(half, j):
        at = aligned(half * part + j * length, length)
        return remote(
            rows_ref.at[at], dy.at[at], c_send.at[half], c_recv.at[half],
            pipe=lax.rem(pi - 1 + np_, np_),
        )

    def down_half(half):
        at = half_of(half)
        return remote(
            rows_ref.at[at], dy.at[at], c_send.at[half], c_recv.at[half],
            pipe=lax.rem(pi - 1 + np_, np_),
        )

    def near_copy(j):
        block = j * fast + fast - 1 - side
        return remote(
            vpart.at[aligned(block * rows, rows, 8)], near_in.at[j], n_send.at[0], n_recv.at[j],
            dp=partner,
        )

    def value_copy(k):
        return remote(
            near_sum.at[lax.rem(line + k, slow)], value_in.at[k], s_send.at[0], s_recv.at[0],
            dp=lax.rem(me + fast * k, n),
        )

    def gain_across(k):
        return remote(gt, gt_in.at[k], t_send.at[k - 1], t_recv.at[k - 1], tensor=lax.rem(ti + k, nt))

    def gain_copy(k):
        peer = lax.rem(me + k, n)
        return remote(gx.at[peer], gx_in.at[k], g_send.at[0], g_recv.at[0], dp=peer)

    gain_all = both_ends(gx_in.at[pl.ds(1, n - 1)], g_send.at[0], g_recv.at[0])
    dy_all = both_ends(
        dy_in.at[:, pl.ds(0, (n - 1) * part)], d_send.at[0], d_recv.at[0]
    )
    near_all = both_ends(near_in, n_send.at[0], n_recv.at[0])
    value_all = both_ends(value_in.at[pl.ds(0, max(1, slow - 1))], s_send.at[0], s_recv.at[0])

    small[0].wait()

    @pl.loop(1, n)
    def _(k):
        bound_copy(k).start()

    @pl.when(last)
    def _():
        for j in range(per_part):
            head_loads[j].wait()
            for k in range(1, nt):
                head_copy(k, j).start()

    wv_load.wait()

    @pl.when(last)
    def _():
        wv_start(True)

    pltpu.make_async_copy(prob, prob, p_load.at[0]).wait()
    for i, group in enumerate(groups):
        for h in range(heads):
            row = h * length
            cells = [
                prob[s, row + b * BAND : row + (b + 1) * BAND, 0:w] for w, b, s in group
            ]
            spare = LANES - sum(w for w, _, _ in group)
            if spare:
                cells.append(jnp.zeros((BAND, spare), jnp.bfloat16))
            first = i * group_rows + h * BAND
            packs[me, first : first + BAND, :] = jnp.concatenate(cells, axis=1)
    send_pack(0, line)

    def half_of(half):
        return aligned(half * part, part)

    def upstream(half, j, block):
        @pl.loop(0, length // BAND)
        def _(r):
            to = aligned(half * part + j * length + r * BAND, BAND)
            rows_in = block(j, aligned(r * BAND, BAND))
            dy[to, :] = (wcol[to, :] * rows_in.astype(jnp.float32)).astype(jnp.bfloat16)

    lots = next(c for c in (4, 2, 1) if width // LANES % c == 0)

    def turn(half):
        at = half_of(half)

        @pl.loop(0, width // (LANES * lots))
        def _(j):
            for i in range(lots):
                to = aligned((j * lots + i) * LANES, LANES)
                turned[to, at] = dy[at, to].T

    def send_dy():
        @pl.loop(1, n)
        def _(k):
            dy_copy(k).start()

    def values_grad(half, source, base):
        at = half_of(half)
        for v in range(value_heads):
            across = []
            for j in range(per_part):
                stacked = jnp.concatenate(
                    [
                        source[
                            h * LANES : (h + 1) * LANES,
                            base + j * length : base + (j + 1) * length,
                        ]
                        for h in range(v * per_value, (v + 1) * per_value)
                    ],
                    axis=1,
                )
                pattern = prob[
                    half * per_part + j, v * per_value * length : (v + 1) * per_value * length, :
                ]
                across.append(jnp.dot(stacked, pattern, preferred_element_type=jnp.float32))
            block = jnp.concatenate(across, axis=1)
            vgt[v * LANES : (v + 1) * LANES, at] = block.astype(jnp.bfloat16)
            vgc[at, aligned(ti * wcols + v * LANES, LANES)] = block.T.astype(jnp.bfloat16)
        for k in range(1, nt):

            @pl.when((pi > 0) | (half == lax.rem(ti + k, nt)))
            def _():
                vg_copy(k, half).start()

    def mixed_grad(half):
        if half is None:
            mg[...] = jnp.dot(wo[...], turned[...], preferred_element_type=jnp.float32).astype(
                jnp.bfloat16
            )
        else:
            for i in range(nt):

                @pl.when(half == i)
                def _():
                    mg_half[...] = jnp.dot(
                        wo[...],
                        turned[:, i * part : (i + 1) * part],
                        preferred_element_type=jnp.float32,
                    ).astype(jnp.bfloat16)

    def pass_on(low, high):
        @pl.loop(low, high)
        def _(k):
            dy_copy(k).wait_recv()
            for j in range(1, nt):
                onward(j, k, ti).start()

    def norm_backward(between=0):
        @pl.loop(0, nt)
        def _(i):
            half = lax.rem(ti + i, nt)

            @pl.when((i == 0) | (pi > 0))
            def _():
                for k in range(1, nt):
                    vg_copy(k, half).wait_recv()
                ng[...] = lax.dot_general(
                    vgc[half_of(half), :],
                    wvc[...],
                    (((1,), (1,)), ((), ())),
                    preferred_element_type=jnp.float32,
                )
                for j in range(per_part):

                    @pl.loop(0, length // BAND)
                    def _(r):
                        here = aligned(j * length + r * BAND, BAND)
                        to = aligned(half * part + j * length + r * BAND, BAND)
                        x = hid[to, :].astype(jnp.float32)
                        inverse = rms[to, :]
                        scaled = ng[here, :] * gain[...]
                        mean = jnp.mean(x * scaled, axis=-1, keepdims=True)
                        grad = inverse * scaled - x * (inverse * inverse * inverse * mean)
                        rows_ref[to, :] = (dy[to, :].astype(jnp.float32) + grad).astype(
                            jnp.bfloat16
                        )

                    if np_ > 1:

                        @pl.when(pi > 0)
                        def _():
                            down_copy(half, j).start()

                if between:

                    @pl.when(i == 0)
                    def _():
                        pass_on(1, between)


        for o in range(own):
            for p in range(micro):
                cot_ref[p, o] = rows_ref[aligned(ti * part + (o * micro + p) * length, length), :]

    def gain_sums():
        whole = gt[...]
        for k in range(1, nt):
            gain_across(k).wait_recv()
            whole = whole + gt_in[k]
        for i in range(n):
            gx[i] = whole[:, i * rows : (i + 1) * rows]

        @pl.loop(1, n)
        def _(k):
            gain_copy(k).start()

    for copy in small[1:]:
        copy.wait()
    pltpu.make_async_copy(hid, hid, h_load.at[0]).wait()

    @pl.loop(0, tokens // BAND)
    def _(i):
        at = aligned(i * BAND, BAND)
        x = hid[at, :].astype(jnp.float32)
        inverse = lax.rsqrt(jnp.mean(x * x, axis=-1, keepdims=True) + EPSILON)
        rms[at, :] = inverse
        normed[at, :] = (x * inverse * gain[...]).astype(jnp.bfloat16)

    values = jnp.dot(normed[...], wvc[:, mine], preferred_element_type=jnp.float32).astype(
        jnp.bfloat16
    )
    for v in range(value_heads):
        packs[me, value_base + v * tokens : value_base + (v + 1) * tokens, :] = values[
            :, v * LANES : (v + 1) * LANES
        ]
    send_pack(1, line)
    wo_load.wait()

    def responses(b):
        spans = jnp.minimum(b[:, 1:2], length) - jnp.maximum(b[:, 0:1], 0)
        return jnp.sum(jnp.maximum(spans, 0), axis=0, keepdims=True)

    total = responses(bound[...])
    bound_all.wait_recv()
    for k in range(1, n):
        total = total + responses(bound_in[k])
    likelihood = LIKELIHOOD_COEF * micro * n / total.astype(jnp.float32)
    along = lax.broadcasted_iota(jnp.int32, (1, length), 1)
    down = lax.broadcasted_iota(jnp.int32, (length, 1), 0)
    for p in range(micro):
        low = bound[p : p + 1, 0:1]
        scores = []
        for c in range(both):
            high = bound[p : p + 1, 1 + c : 2 + c]
            inside = jnp.where((along >= low) & (along < high), policy[p, c : c + 1, :], 0.0)
            scores.append(
                jnp.sum(inside, axis=-1, keepdims=True) - refer[p : p + 1, c : c + 1]
            )
        margin = DPO_BETA * (scores[0] - scores[1])
        pair = jax.nn.sigmoid(-margin)
        for c in range(both):
            high = bound[p : p + 1, 1 + c : 2 + c]
            weight = -DPO_BETA * pair - likelihood if c == 0 else DPO_BETA * pair
            inside = (down >= low) & (down < high)
            wcol[(c * micro + p) * length : (c * micro + p + 1) * length, :] = jnp.where(
                inside, jnp.broadcast_to(weight, (length, 1)), 0.0
            )

    def mix(src, slot):
        for v in range(value_heads):
            for i, group in enumerate(groups):
                first = i * group_rows + v * per_value * BAND
                pattern = packs[src, first : first + per_value * BAND, :]
                blocks, start = [], 0
                for w, b, s in group:
                    key = value_base + v * tokens + s * length
                    cells = [packs[src, key : key + w, :]]
                    if start:
                        cells.insert(0, jnp.zeros((start, LANES), jnp.bfloat16))
                    if start + w < LANES:
                        cells.append(jnp.zeros((LANES - start - w, LANES), jnp.bfloat16))
                    blocks.append(jnp.concatenate(cells, axis=0) if len(cells) > 1 else cells[0])
                    start += w
                product = jnp.dot(
                    pattern,
                    jnp.concatenate(blocks, axis=1) if len(blocks) > 1 else blocks[0],
                    preferred_element_type=jnp.float32,
                ).astype(jnp.bfloat16)
                for j, (w, b, s) in enumerate(group):
                    row = s * length + b * BAND
                    for h in range(per_value):
                        column = (v * per_value + h) * LANES
                        mixed[
                            aligned(slot * tokens + row, BAND), column : column + LANES
                        ] = product[
                            h * BAND : (h + 1) * BAND, j * LANES : (j + 1) * LANES
                        ]

    def turn_wv():
        @pl.loop(0, width // (LANES * lots))
        def _(j):
            for i in range(lots):
                to = aligned((j * lots + i) * LANES, LANES)
                wvt[:, to] = wvc[to, mine].T

    def value_part():
        for v in range(value_heads):
            ng[0:LANES, :] = jnp.dot(
                vgt[v * LANES : (v + 1) * LANES, :],
                normed[...],
                preferred_element_type=jnp.float32,
            )
            part_gain = jnp.sum(
                ng[0:LANES, :] * wvt[v * LANES : (v + 1) * LANES, :].astype(jnp.float32),
                axis=0,
                keepdims=True,
            )
            gt[...] = part_gain if v == 0 else gt[...] + part_gain

            @pl.loop(0, width // (LANES * lots))
            def _(j):
                for i in range(lots):
                    to = aligned((j * lots + i) * LANES, LANES)
                    vpart[to, v * LANES : (v + 1) * LANES] = (
                        ng[0:LANES, to].astype(jnp.bfloat16).T
                    )

        if fast > 1:

            @pl.loop(1, slow + 1)
            def _(k):
                near_copy(lax.rem(line + k, slow)).start()

        gt[...] = gt[...] / gain[...]
        for k in range(1, nt):
            gain_across(k).start()

    def near_sums():
        @pl.loop(1, slow + 1)
        def _(k):
            j = lax.rem(line + k, slow)
            near = vpart[aligned((j * fast + side) * rows, rows, 8), :].astype(jnp.float32)
            if fast > 1:
                near_copy(j).wait_recv()
                near = near + near_in[j].astype(jnp.float32)
            near_sum[j] = near.astype(jnp.bfloat16)

            @pl.when(k < slow)
            def _():
                value_copy(k).start()

    def pack_waits():
        if fast > 1:

            y_all.wait_recv()

    keep = mixed.shape[0] == n * tokens
    span = fast * tokens

    def mix_side(f):
        if keep:

            @pl.loop(0, slow)
            def _(b):
                mix(b * fast + f, b * fast + f)

    def products(low, high):
        @pl.loop(low, high)
        def _(d):
            b = lax.rem(line - d + slow, slow)
            if not keep:
                for f in range(fast):
                    mix(b * fast + f, f)
            for f in range(fast):

                @pl.when((d > 0) | (f > 0))
                def _():
                    for j in range(1, nt):
                        onward(j, d * fast + f, lax.rem(ti - j + nt, nt)).wait_recv()

            term = jnp.dot(
                dy_in[:, aligned(b * span, span)],
                mixed[aligned(b * span, span), :] if keep else mixed[...],
                preferred_element_type=jnp.float32,
            )

            @pl.when(d == 0)
            def _():
                out_ref[...] = term

            @pl.when(d > 0)
            def _():
                out_ref[...] += term

    def own_rows():
        dy_in[:, aligned(me * tokens, tokens)] = turned[aligned(me * rows, rows, 8), :]

    def value_final():
        value_ref[...] = near_sum[line].astype(jnp.float32)

        if slow > 1:
            value_all.wait_recv()

        @pl.loop(1, slow)
        def _(k):
            value_ref[...] += value_in[k].astype(jnp.float32)

    @pl.when(last)
    def _():
        for j in range(per_part):
            upstream(ti, j, lambda s, at: head[s, at, :])
        turn(ti)
        mixed_grad(ti)
        values_grad(ti, mg_half, 0)
        relay((0, 1), 1, min(2, slow))
        turn_wv()
        relay((0, 1), min(2, slow), min(3, slow))
        send_dy()
        for i in range(1, nt):
            half = lax.rem(ti - i + nt, nt)
            for j in range(per_part):
                head_copy(i, j).wait_recv()
                upstream(half, j, lambda s, at: head_in[i, s, at, :])
            turn(half)
            mixed_grad(half)
            values_grad(half, mg_half, 0)
        value_part()
        relay((0, 1), min(3, slow), slow)
        wv_arrive(True)
        go_on()
        norm_backward(min(2, n))
        pass_on(min(2, n), n)
        gain_sums()
        pack_waits()
        own_rows()
        for f in range(fast):
            mix_side(f)
        products(0, min(2, slow))
        near_sums()
        products(min(2, slow), slow)
        value_final()

    if np_ > 1:

        @pl.when(jnp.logical_not(last))
        def _():
            relay((0, 1), 1, slow)
            mix_side(side)
            turn_wv()
            pl.semaphore_wait(go, 1)
            wv_start(False)
            for i in range(nt):
                half = lax.rem(ti + i, nt)
                down_half(half).wait_recv()
                turn(half)
                if i == 0:
                    send_dy()
            wv_arrive(False)
            mixed_grad(None)
            for i in range(nt):
                values_grad(i, mg, i * part)
            value_part()
            pass_on(1, min(4, n))
            pack_waits()
            own_rows()
            for f in range(1, fast):
                mix_side(lax.rem(side + f, fast))
            pass_on(min(4, n), n)
            go_on()
            wv_wait()
            norm_backward()
            gain_sums()
            near_sums()
            products(0, slow)
            value_final()

    gain_sum = gx[me]
    gain_all.wait_recv()
    for k in range(1, n):
        gain_sum = gain_sum + gx_in[k]
    gain_out_ref[...] = gain_sum

    bound_all.wait_send()
    dy_all.wait_send()
    gain_all.wait_send()
    for j in range(1, nt):
        both_ends(
            dy_in.at[:, pl.ds(0, (n - 1) * part)], o_send.at[j - 1], o_recv.at[j - 1, 0]
        ).wait_send()
    if slow > 1:
        value_all.wait_send()
    if fast > 1:
        near_all.wait_send()
        y_all.wait_send()

    @pl.loop(0, slow)
    def _(b):
        for q in range(2):

            @pl.when((line < slow - 1) & (b <= line))
            def _():
                right_copy(q, b).wait_send()

            @pl.when((line > 0) & (b >= line))
            def _():
                left_copy(q, b).wait_send()

    for k in range(1, nt):
        gain_across(k).wait_send()
        for half in range(nt):

            @pl.when((pi > 0) | (half == lax.rem(ti + k, nt)))
            def _():
                vg_copy(k, half).wait_send()

    @pl.when(last)
    def _():
        wv_sent(True)
        for k in range(1, nt):
            for j in range(per_part):
                head_copy(k, j).wait_send()

    if np_ > 1:

        @pl.when(jnp.logical_not(last))
        def _():
            wv_sent(False)

    if np_ > 1:

        @pl.when(pi > 0)
        def _():
            for half in range(nt):
                down_half(half).wait_send()


def layer(sizes, hidden, probs, gain, wv, wo, head, policy, refer, bounds):
    n, nt, _ = sizes
    micro, both, length, width = hidden.shape
    own = head.shape[1]
    tokens = micro * both * length
    sequences = micro * both
    columns = wo.shape[0]
    heads = columns // LANES
    wcols = wv.shape[1]
    rows = width // n
    part = tokens // nt
    fast = 2 if n % 2 == 0 else 1
    slow = n // fast
    pack_rows = (
        len(bands(sequences, length)) * heads * BAND + wcols // LANES * tokens
    )
    per_part = part // length
    keep = n * tokens * columns <= 2**22
    vmem = pl.BlockSpec(memory_space=pltpu.VMEM)
    dma = pltpu.SemaphoreType.DMA
    bf, f32, i32 = jnp.bfloat16, jnp.float32, jnp.int32
    return pl.pallas_call(
        functools.partial(layer_kernel, sizes),
        out_shape=(
            pltpu.VMEM((micro, own, length, width), bf),
            pltpu.VMEM((rows, wcols), f32),
            pltpu.VMEM((rows, columns), f32),
            pltpu.VMEM((1, rows), f32),
        ),
        in_specs=[pl.BlockSpec(memory_space=pl.ANY)] * 9,
        out_specs=(vmem,) * 4,
        scratch_shapes=[
            pltpu.VMEM((tokens, width), bf),
            pltpu.VMEM((sequences, heads * length, length), bf),
            pltpu.VMEM((1, width), f32),
            pltpu.VMEM((width, nt * wcols), bf),
            pltpu.VMEM((columns, width), bf),
            pltpu.VMEM((own * micro, length, width), bf),
            pltpu.VMEM((nt, own * micro, length, width), bf),
            pltpu.VMEM(policy.shape, f32),
            pltpu.VMEM(refer.shape, f32),
            pltpu.VMEM(bounds.shape, i32),
            pltpu.VMEM((n,) + bounds.shape, i32),
            pltpu.VMEM((tokens, 1), f32),
            pltpu.VMEM((tokens, width), bf),
            pltpu.VMEM((tokens, 1), f32),
            pltpu.VMEM((n, pack_rows, LANES), bf),
            pltpu.VMEM((tokens, width), bf),
            pltpu.VMEM((width, tokens), bf),
            pltpu.VMEM((columns, tokens), bf),
            pltpu.VMEM((columns, part), bf),
            pltpu.VMEM((wcols, tokens), bf),
            pltpu.VMEM((tokens, nt * wcols), bf),
            pltpu.VMEM((part, width), f32),
            pltpu.VMEM((tokens, width), bf),
            pltpu.VMEM((width, wcols), bf),
            pltpu.VMEM((slow, rows, wcols), bf),
            pltpu.VMEM((slow, rows, wcols), bf),
            pltpu.VMEM((slow, rows, wcols), bf),
            pltpu.VMEM((rows, n * tokens), bf),
            pltpu.VMEM(((n if keep else fast) * tokens, columns), bf),
            pltpu.VMEM((wcols, width), bf),
            pltpu.VMEM((1, width), f32),
            pltpu.VMEM((nt, 1, width), f32),
            pltpu.VMEM((n, 1, rows), f32),
            pltpu.VMEM((n, 1, rows), f32),
            dma((6 + own * micro,)),
            dma((1,)),
            dma((1,)),
            dma((1,)),
            dma((1,)),
            dma((nt - 1, own * micro)),
            dma((nt - 1, own * micro)),
            dma((nt - 1, 2)),
            dma((nt - 1, 2)),
            dma((nt - 1,)),
            dma((nt - 1,)),
            dma((2, slow)),
            dma((2, slow)),
            dma((2, slow)),
            dma((1,)),
            dma((1,)),
            dma((1,)),
            dma((n - 1,)),
            dma((nt - 1,)),
            dma((nt - 1, n - 1)),
            dma((nt - 1, nt)),
            dma((nt - 1, nt)),
            dma((nt,)),
            dma((nt,)),
            dma((1,)),
            dma((slow,)),
            dma((1,)),
            dma((1,)),
            dma((1,)),
            dma((1,)),
            dma((nt - 1,)),
            dma((nt - 1,)),
            pltpu.SemaphoreType.REGULAR,
        ],
        compiler_params=pltpu.CompilerParams(
            collective_id=0, has_side_effects=True, vmem_limit_bytes=52 * 2**20
        ),
        name="layer",
    )(hidden, probs, gain, wv, wo, head, policy, refer, bounds)


def finish_kernel(*refs):
    count = len(refs) // 2
    sem = refs[-1]
    copies = [
        pltpu.make_async_copy(refs[i], refs[count + i], sem.at[i]) for i in range(count)
    ]
    for copy in copies:
        copy.start()
    for copy in copies:
        copy.wait()


def finish(arrays):
    return pl.pallas_call(
        finish_kernel,
        out_shape=tuple(jax.ShapeDtypeStruct(a.shape, a.dtype) for a in arrays),
        in_specs=[pl.BlockSpec(memory_space=pltpu.VMEM)] * len(arrays),
        out_specs=(pl.BlockSpec(memory_space=pl.ANY),) * len(arrays),
        scratch_shapes=[pltpu.SemaphoreType.DMA((len(arrays),))],
        compiler_params=pltpu.CompilerParams(vmem_limit_bytes=2**20),
        name="finish",
    )(*(pltpu.with_memory_space_constraint(a, pltpu.VMEM) for a in arrays))


def body(
    hidden_in,
    attention_probs,
    norm_gain,
    value_weight,
    output_weight,
    head_grad,
    policy_logprob,
    reference_logprob,
    sequence_bounds,
):
    sizes = tuple(lax.axis_size(a) for a in ("dp", "tensor", "pipe"))
    micro, both, heads, length, _ = attention_probs.shape[1:]
    cotangent, value, output, gain = finish(layer(
        sizes,
        hidden_in[0],
        attention_probs[0].reshape(micro, both, heads * length, length),
        norm_gain,
        value_weight[0],
        output_weight[0],
        head_grad,
        policy_logprob,
        reference_logprob,
        sequence_bounds,
    ))
    return (cotangent[None], value[None], output[None], gain)


def solution(mesh):
    in_specs = (
        P("pipe", "dp", None, None, None),
        P("pipe", "dp", None, "tensor", None, None),
        P("pipe", None),
        P("pipe", None, "tensor"),
        P("pipe", "tensor", None),
        P("dp", "tensor", None, None),
        P("dp", None, None),
        P("dp", None),
        P("dp", None),
    )
    out_specs = (
        P("pipe", "dp", "tensor", None, None),
        P("pipe", "dp", "tensor"),
        P("pipe", "dp", "tensor"),
        P("pipe", "dp"),
    )
    return jax.shard_map(body, mesh=mesh, in_specs=in_specs, out_specs=out_specs, check_vma=False)
```

```python
import functools

import jax
import jax.numpy as jnp
from jax import lax
from jax.experimental import pallas as pl
from jax.experimental.pallas import tpu as pltpu
from jax.sharding import PartitionSpec as P

LANES = 128
BAND = 16
MESH = pl.DeviceIdType.MESH

EPSILON = 1e-06
DPO_BETA = 0.25
LIKELIHOOD_COEF = 0.2


def greet(peers):
    barrier = pltpu.get_barrier_semaphore()
    total = 0
    for axis, n in peers:
        me = lax.axis_index(axis)

        @pl.loop(1, n)
        def _(k):
            pl.semaphore_signal(
                barrier, inc=1, device_id={axis: lax.rem(me + k, n)}, device_id_type=MESH
            )

        total += n - 1
    pl.semaphore_wait(barrier, total)


def remote(src, dst, send_sem, recv_sem, **device):
    return pltpu.make_async_remote_copy(
        src_ref=src,
        dst_ref=dst,
        send_sem=send_sem,
        recv_sem=recv_sem,
        device_id=device,
        device_id_type=MESH,
    )


def aligned(start, size, to=None):
    return pl.ds(pl.multiple_of(start, to or size), size)


def bands(sequences, length):
    todo = sorted(
        ((b + 1) * BAND, b, s) for b in range(length // BAND) for s in range(sequences)
    )
    groups = []
    for width, b, s in sorted(todo, key=lambda t: (-t[0], t[2])):
        for group in groups:
            start = sum(w for w, _, _ in group)
            if start + width <= LANES:
                group.append((width, b, s))
                break
        else:
            groups.append([(width, b, s)])
    return groups


def layer_kernel(
    sizes,
    hidden_hbm,
    probs_hbm,
    gain_hbm,
    wv_hbm,
    wo_hbm,
    head_hbm,
    policy_hbm,
    refer_hbm,
    bounds_hbm,
    cot_ref,
    value_ref,
    out_ref,
    gain_out_ref,
    hid,
    prob,
    gain,
    wvc,
    wo,
    head,
    head_in,
    policy,
    refer,
    bound,
    bound_in,
    wcol,
    normed,
    rms,
    packs,
    dy,
    turned,
    mg,
    mg_half,
    vgt,
    vgc,
    ng,
    rows_ref,
    vpart,
    near_in,
    near_sum,
    value_in,
    dy_in,
    mixed,
    wvt,
    gt,
    gt_in,
    gx,
    gx_in,
    load_sem,
    h_load,
    p_load,
    b_send,
    b_recv,
    h_send,
    h_recv,
    w_send,
    w_recv,
    a_send,
    a_recv,
    r_send,
    l_send,
    z_recv,
    y_send,
    y_recv,
    d_send,
    d_recv,
    o_send,
    o_recv,
    v_send,
    v_recv,
    c_send,
    c_recv,
    n_send,
    n_recv,
    s_send,
    s_recv,
    g_send,
    g_recv,
    t_send,
    t_recv,
    go,
    back,
):
    n, nt, np_ = sizes
    me, ti, pi = lax.axis_index("dp"), lax.axis_index("tensor"), lax.axis_index("pipe")
    micro, both, length, width = hidden_hbm.shape
    own = head_hbm.shape[1]
    tokens = micro * both * length
    part = tokens // nt
    per_part = part // length
    columns = wo.shape[0]
    heads = columns // LANES
    wcols = wv_hbm.shape[1]
    value_heads = wcols // LANES
    per_value = heads // value_heads
    rows = width // n
    fast = 2 if n % 2 == 0 else 1
    slow = n // fast
    line, side = lax.div(me, fast), lax.rem(me, fast)
    partner = me + 1 - 2 * side
    last = pi == np_ - 1
    groups = bands(micro * both, length)
    group_rows = heads * BAND
    value_base = len(groups) * group_rows
    pack_parts = ((0, value_base), (value_base, tokens * value_heads))

    def load(src, dst, i):
        return pltpu.make_async_copy(src, dst, load_sem.at[i])

    mine = aligned(ti * wcols, wcols)
    small = [
        load(bounds_hbm, bound, 0),
        load(policy_hbm, policy, 1),
        load(refer_hbm, refer, 2),
        load(gain_hbm, gain, 3),
    ]
    wv_load = load(wv_hbm, wvc.at[:, mine], 4)
    wo_load = load(wo_hbm, wo, 5)
    hid_loads, prob_loads, head_loads = [], [], []
    for c in range(both):
        for p in range(micro):
            s = c * micro + p
            hid_loads.append(
                pltpu.make_async_copy(
                    hidden_hbm.at[p, c], hid.at[pl.ds(s * length, length)], h_load.at[0]
                )
            )
            prob_loads.append(
                pltpu.make_async_copy(probs_hbm.at[p, c], prob.at[s], p_load.at[0])
            )
    for o in range(own):
        for p in range(micro):
            head_loads.append(load(head_hbm.at[p, o], head.at[o * micro + p], 6 + o * micro + p))
    small[0].start()

    @pl.when(last)
    def _():
        for copy in head_loads:
            copy.start()

    for copy in hid_loads + small[1:]:
        copy.start()
    wv_load.start()
    for copy in prob_loads:
        copy.start()
    wo_load.start()
    greet((("dp", n), ("tensor", nt), ("pipe", np_)))

    def both_ends(block, send, recv):
        return remote(block, block, send, recv, dp=lax.rem(me + 1, n))

    def bound_copy(k):
        return remote(bound, bound_in.at[k], b_send.at[0], b_recv.at[0], dp=lax.rem(me + k, n))

    bound_all = both_ends(bound_in.at[pl.ds(1, n - 1)], b_send.at[0], b_recv.at[0])

    def head_copy(k, j):
        return remote(
            head.at[j], head_in.at[k, j], h_send.at[k - 1, j], h_recv.at[k - 1, j],
            tensor=lax.rem(ti + k, nt),
        )

    quarter = width // 4

    def wv_copy(k, piece):
        block = wvc.at[aligned(piece * quarter, quarter, BAND), mine]
        return remote(
            block, block, w_send.at[k - 1, 1], w_recv.at[k - 1, 1], tensor=lax.rem(ti + k, nt)
        )

    def wv_other(k):
        return wvc.at[pl.ds(0, width // 2), aligned(lax.rem(ti - k + nt, nt) * wcols, wcols)]

    def wv_direct(k, i):
        block = wvc.at[pl.ds(*((0, 3 * quarter), (3 * quarter, quarter))[i]), mine]
        return remote(
            block, block, w_send.at[k - 1, i], w_recv.at[k - 1, i], tensor=lax.rem(ti + k, nt)
        )

    def wv_across(k, piece):
        at = aligned(lax.rem(ti - k + nt, nt) * wcols, wcols)
        block = wvc.at[aligned(piece * quarter, quarter, BAND), at]
        return remote(block, block, a_send.at[k - 1], a_recv.at[k - 1], dp=partner)

    def wv_half(k):
        return remote(
            wv_other(k), wv_other(k), w_send.at[k - 1, 1], w_recv.at[k - 1, 1],
            tensor=lax.rem(ti + k, nt),
        )

    pieces = (side, 2 + side)

    def wv_start(direct):
        for k in range(1, nt):
            if direct or fast == 1:
                wv_direct(k, 0).start()
                if not direct:
                    wv_direct(k, 1).start()
            else:
                for piece in pieces:
                    wv_copy(k, piece).start()

    def wv_arrive(direct):
        for k in range(1, nt):
            if direct or fast == 1:
                wv_direct(k, 0).wait_recv()
                wv_direct(k, 1).wait_recv()
            else:
                wv_half(k).wait_recv()
                for piece in pieces:
                    wv_across(k, piece).start()

    def wv_across_all(k):
        return both_ends(wv_other(k), a_send.at[k - 1], a_recv.at[k - 1])

    def wv_wait():
        if fast > 1:
            for k in range(1, nt):
                wv_across_all(k).wait_recv()

    def wv_sent(direct):
        for k in range(1, nt):
            if direct or fast == 1:
                wv_direct(k, 0).wait_send()
                if not direct:
                    wv_direct(k, 1).wait_send()
            else:
                wv_half(k).wait_send()
                wv_across_all(k).wait_send()

    def pass_turn():
        if np_ > 1:

            @pl.when(pi > 0)
            def _():
                pl.semaphore_wait(back, 1)

    def go_on():
        if np_ > 1:

            @pl.when(pi > 0)
            def _():
                pl.semaphore_signal(go, inc=1, device_id={"pipe": pi - 1}, device_id_type=MESH)

    def vg_copy(k, half):
        block = vgc.at[aligned(half * part, part), mine]
        return remote(
            block, block, v_send.at[k - 1, half], v_recv.at[k - 1, half], tensor=lax.rem(ti + k, nt)
        )

    def pack_copy(q, b, send, peer):
        block = packs.at[b * fast + side, pl.ds(*pack_parts[q])]
        return remote(block, block, send.at[q, b], z_recv.at[q, b], dp=peer)

    def right_copy(q, b):
        return pack_copy(q, b, r_send, lax.rem(me + fast, n))

    def left_copy(q, b):
        return pack_copy(q, b, l_send, lax.rem(me - fast + n, n))

    def y_copy(q, b):
        block = packs.at[b * fast + side, pl.ds(*pack_parts[q])]
        return remote(block, block, y_send.at[0], y_recv.at[0], dp=partner)

    y_all = both_ends(packs.at[pl.ds(0, slow)], y_send.at[0], y_recv.at[0])

    def send_pack(q, b):
        @pl.when((line < slow - 1) & (b <= line))
        def _():
            right_copy(q, b).start()

        @pl.when((line > 0) & (b >= line))
        def _():
            left_copy(q, b).start()

        if fast > 1:
            y_copy(q, b).start()

    def relay(parts, low, high):
        @pl.loop(low, high)
        def _(d):
            for q in parts:

                @pl.when(line >= d)
                def _():
                    right_copy(q, line - d).wait_recv()
                    send_pack(q, line - d)

                @pl.when(line + d < slow)
                def _():
                    left_copy(q, line + d).wait_recv()
                    send_pack(q, line + d)

    def ahead(e):
        d, f = lax.div(e, fast), lax.rem(e, fast)
        there = lax.rem(line + d, slow) * fast + lax.rem(side + f, fast)
        back = lax.rem(line - d + slow, slow) * fast + lax.rem(side - f + fast, fast)
        return there, back

    def dy_copy(e):
        peer = ahead(e)[0]
        return remote(
            turned.at[aligned(peer * rows, rows, 8), aligned(ti * part, part)],
            dy_in.at[:, aligned(me * tokens + ti * part, part)],
            d_send.at[0], d_recv.at[e - 1], dp=peer,
        )

    def onward(j, e, half):
        block = dy_in.at[:, aligned(ahead(e)[1] * tokens + half * part, part)]
        return remote(
            block, block, o_send.at[j - 1], o_recv.at[j - 1, e - 1], tensor=lax.rem(ti + j, nt)
        )

    def down_copy(half, j):
        at = aligned(half * part + j * length, length)
        return remote(
            rows_ref.at[at], dy.at[at], c_send.at[half], c_recv.at[half],
            pipe=lax.rem(pi - 1 + np_, np_),
        )

    def down_half(half):
        at = half_of(half)
        return remote(
            rows_ref.at[at], dy.at[at], c_send.at[half], c_recv.at[half],
            pipe=lax.rem(pi - 1 + np_, np_),
        )

    def near_copy(j):
        block = j * fast + fast - 1 - side
        return remote(
            vpart.at[aligned(block * rows, rows, 8)], near_in.at[j], n_send.at[0], n_recv.at[j],
            dp=partner,
        )

    def value_copy(k):
        return remote(
            near_sum.at[lax.rem(line + k, slow)], value_in.at[k], s_send.at[0], s_recv.at[0],
            dp=lax.rem(me + fast * k, n),
        )

    def gain_across(k):
        return remote(gt, gt_in.at[k], t_send.at[k - 1], t_recv.at[k - 1], tensor=lax.rem(ti + k, nt))

    def gain_copy(k):
        peer = lax.rem(me + k, n)
        return remote(gx.at[peer], gx_in.at[k], g_send.at[0], g_recv.at[0], dp=peer)

    gain_all = both_ends(gx_in.at[pl.ds(1, n - 1)], g_send.at[0], g_recv.at[0])
    dy_all = both_ends(
        dy_in.at[:, pl.ds(0, (n - 1) * part)], d_send.at[0], d_recv.at[0]
    )
    near_all = both_ends(near_in, n_send.at[0], n_recv.at[0])
    value_all = both_ends(value_in.at[pl.ds(0, max(1, slow - 1))], s_send.at[0], s_recv.at[0])

    small[0].wait()

    @pl.loop(1, n)
    def _(k):
        bound_copy(k).start()

    @pl.when(last)
    def _():
        for j in range(per_part):
            head_loads[j].wait()
            for k in range(1, nt):
                head_copy(k, j).start()

    wv_load.wait()

    @pl.when(last)
    def _():
        wv_start(True)

    pltpu.make_async_copy(prob, prob, p_load.at[0]).wait()
    for i, group in enumerate(groups):
        for h in range(heads):
            row = h * length
            cells = [
                prob[s, row + b * BAND : row + (b + 1) * BAND, 0:w] for w, b, s in group
            ]
            spare = LANES - sum(w for w, _, _ in group)
            if spare:
                cells.append(jnp.zeros((BAND, spare), jnp.bfloat16))
            first = i * group_rows + h * BAND
            packs[me, first : first + BAND, :] = jnp.concatenate(cells, axis=1)
    send_pack(0, line)

    def half_of(half):
        return aligned(half * part, part)

    def upstream(half, j, block):
        @pl.loop(0, length // BAND)
        def _(r):
            to = aligned(half * part + j * length + r * BAND, BAND)
            rows_in = block(j, aligned(r * BAND, BAND))
            dy[to, :] = (wcol[to, :] * rows_in.astype(jnp.float32)).astype(jnp.bfloat16)

    lots = next(c for c in (4, 2, 1) if width // LANES % c == 0)

    def turn(half):
        at = half_of(half)

        @pl.loop(0, width // (LANES * lots))
        def _(j):
            for i in range(lots):
                to = aligned((j * lots + i) * LANES, LANES)
                turned[to, at] = dy[at, to].T

    def send_dy():
        @pl.loop(1, n)
        def _(k):
            dy_copy(k).start()

    def values_grad(half, source, base):
        at = half_of(half)
        for v in range(value_heads):
            across = []
            for j in range(per_part):
                stacked = jnp.concatenate(
                    [
                        source[
                            h * LANES : (h + 1) * LANES,
                            base + j * length : base + (j + 1) * length,
                        ]
                        for h in range(v * per_value, (v + 1) * per_value)
                    ],
                    axis=1,
                )
                pattern = prob[
                    half * per_part + j, v * per_value * length : (v + 1) * per_value * length, :
                ]
                across.append(jnp.dot(stacked, pattern, preferred_element_type=jnp.float32))
            block = jnp.concatenate(across, axis=1)
            vgt[v * LANES : (v + 1) * LANES, at] = block.astype(jnp.bfloat16)
            vgc[at, aligned(ti * wcols + v * LANES, LANES)] = block.T.astype(jnp.bfloat16)
        for k in range(1, nt):

            @pl.when((pi > 0) | (half == lax.rem(ti + k, nt)))
            def _():
                vg_copy(k, half).start()

    def mixed_grad(half):
        if half is None:
            mg[...] = jnp.dot(wo[...], turned[...], preferred_element_type=jnp.float32).astype(
                jnp.bfloat16
            )
        else:
            for i in range(nt):

                @pl.when(half == i)
                def _():
                    mg_half[...] = jnp.dot(
                        wo[...],
                        turned[:, i * part : (i + 1) * part],
                        preferred_element_type=jnp.float32,
                    ).astype(jnp.bfloat16)

    def pass_on(low, high):
        @pl.loop(low, high)
        def _(k):
            dy_copy(k).wait_recv()
            for j in range(1, nt):
                onward(j, k, ti).start()

    def norm_backward(between=0):
        @pl.loop(0, nt)
        def _(i):
            half = lax.rem(ti + i, nt)

            @pl.when((i == 0) | (pi > 0))
            def _():
                for k in range(1, nt):
                    vg_copy(k, half).wait_recv()
                ng[...] = lax.dot_general(
                    vgc[half_of(half), :],
                    wvc[...],
                    (((1,), (1,)), ((), ())),
                    preferred_element_type=jnp.float32,
                )
                for j in range(per_part):

                    @pl.loop(0, length // BAND)
                    def _(r):
                        here = aligned(j * length + r * BAND, BAND)
                        to = aligned(half * part + j * length + r * BAND, BAND)
                        x = hid[to, :].astype(jnp.float32)
                        inverse = rms[to, :]
                        scaled = ng[here, :] * gain[...]
                        mean = jnp.mean(x * scaled, axis=-1, keepdims=True)
                        grad = inverse * scaled - x * (inverse * inverse * inverse * mean)
                        rows_ref[to, :] = (dy[to, :].astype(jnp.float32) + grad).astype(
                            jnp.bfloat16
                        )

                    if np_ > 1:

                        @pl.when(pi > 0)
                        def _():
                            down_copy(half, j).start()

                if between:

                    @pl.when(i == 0)
                    def _():
                        pass_on(1, between)


        for o in range(own):
            for p in range(micro):
                cot_ref[p, o] = rows_ref[aligned(ti * part + (o * micro + p) * length, length), :]

    def gain_sums():
        whole = gt[...]
        for k in range(1, nt):
            gain_across(k).wait_recv()
            whole = whole + gt_in[k]
        for i in range(n):
            gx[i] = whole[:, i * rows : (i + 1) * rows]

        @pl.loop(1, n)
        def _(k):
            gain_copy(k).start()

    for copy in small[1:]:
        copy.wait()
    pltpu.make_async_copy(hid, hid, h_load.at[0]).wait()

    @pl.loop(0, tokens // BAND)
    def _(i):
        at = aligned(i * BAND, BAND)
        x = hid[at, :].astype(jnp.float32)
        inverse = lax.rsqrt(jnp.mean(x * x, axis=-1, keepdims=True) + EPSILON)
        rms[at, :] = inverse
        normed[at, :] = (x * inverse * gain[...]).astype(jnp.bfloat16)

    values = jnp.dot(normed[...], wvc[:, mine], preferred_element_type=jnp.float32).astype(
        jnp.bfloat16
    )
    for v in range(value_heads):
        packs[me, value_base + v * tokens : value_base + (v + 1) * tokens, :] = values[
            :, v * LANES : (v + 1) * LANES
        ]
    send_pack(1, line)
    wo_load.wait()

    def responses(b):
        spans = jnp.minimum(b[:, 1:2], length) - jnp.maximum(b[:, 0:1], 0)
        return jnp.sum(jnp.maximum(spans, 0), axis=0, keepdims=True)

    total = responses(bound[...])
    bound_all.wait_recv()
    for k in range(1, n):
        total = total + responses(bound_in[k])
    likelihood = LIKELIHOOD_COEF * micro * n / total.astype(jnp.float32)
    along = lax.broadcasted_iota(jnp.int32, (1, length), 1)
    down = lax.broadcasted_iota(jnp.int32, (length, 1), 0)
    for p in range(micro):
        low = bound[p : p + 1, 0:1]
        scores = []
        for c in range(both):
            high = bound[p : p + 1, 1 + c : 2 + c]
            inside = jnp.where((along >= low) & (along < high), policy[p, c : c + 1, :], 0.0)
            scores.append(
                jnp.sum(inside, axis=-1, keepdims=True) - refer[p : p + 1, c : c + 1]
            )
        margin = DPO_BETA * (scores[0] - scores[1])
        pair = jax.nn.sigmoid(-margin)
        for c in range(both):
            high = bound[p : p + 1, 1 + c : 2 + c]
            weight = -DPO_BETA * pair - likelihood if c == 0 else DPO_BETA * pair
            inside = (down >= low) & (down < high)
            wcol[(c * micro + p) * length : (c * micro + p + 1) * length, :] = jnp.where(
                inside, jnp.broadcast_to(weight, (length, 1)), 0.0
            )

    def mix(src, slot):
        for v in range(value_heads):
            for i, group in enumerate(groups):
                first = i * group_rows + v * per_value * BAND
                pattern = packs[src, first : first + per_value * BAND, :]
                blocks, start = [], 0
                for w, b, s in group:
                    key = value_base + v * tokens + s * length
                    cells = [packs[src, key : key + w, :]]
                    if start:
                        cells.insert(0, jnp.zeros((start, LANES), jnp.bfloat16))
                    if start + w < LANES:
                        cells.append(jnp.zeros((LANES - start - w, LANES), jnp.bfloat16))
                    blocks.append(jnp.concatenate(cells, axis=0) if len(cells) > 1 else cells[0])
                    start += w
                product = jnp.dot(
                    pattern,
                    jnp.concatenate(blocks, axis=1) if len(blocks) > 1 else blocks[0],
                    preferred_element_type=jnp.float32,
                ).astype(jnp.bfloat16)
                for j, (w, b, s) in enumerate(group):
                    row = s * length + b * BAND
                    for h in range(per_value):
                        column = (v * per_value + h) * LANES
                        mixed[
                            aligned(slot * tokens + row, BAND), column : column + LANES
                        ] = product[
                            h * BAND : (h + 1) * BAND, j * LANES : (j + 1) * LANES
                        ]

    def turn_wv():
        @pl.loop(0, width // (LANES * lots))
        def _(j):
            for i in range(lots):
                to = aligned((j * lots + i) * LANES, LANES)
                wvt[:, to] = wvc[to, mine].T

    def value_part():
        for v in range(value_heads):
            ng[0:LANES, :] = jnp.dot(
                vgt[v * LANES : (v + 1) * LANES, :],
                normed[...],
                preferred_element_type=jnp.float32,
            )
            part_gain = jnp.sum(
                ng[0:LANES, :] * wvt[v * LANES : (v + 1) * LANES, :].astype(jnp.float32),
                axis=0,
                keepdims=True,
            )
            gt[...] = part_gain if v == 0 else gt[...] + part_gain

            @pl.loop(0, width // (LANES * lots))
            def _(j):
                for i in range(lots):
                    to = aligned((j * lots + i) * LANES, LANES)
                    vpart[to, v * LANES : (v + 1) * LANES] = (
                        ng[0:LANES, to].astype(jnp.bfloat16).T
                    )

        if fast > 1:

            @pl.loop(1, slow + 1)
            def _(k):
                near_copy(lax.rem(line + k, slow)).start()

        gt[...] = gt[...] / gain[...]
        for k in range(1, nt):
            gain_across(k).start()

    def near_sums():
        @pl.loop(1, slow + 1)
        def _(k):
            j = lax.rem(line + k, slow)
            near = vpart[aligned((j * fast + side) * rows, rows, 8), :].astype(jnp.float32)
            if fast > 1:
                near_copy(j).wait_recv()
                near = near + near_in[j].astype(jnp.float32)
            near_sum[j] = near.astype(jnp.bfloat16)

            @pl.when(k < slow)
            def _():
                value_copy(k).start()

    def pack_waits():
        if fast > 1:

            y_all.wait_recv()

    keep = mixed.shape[0] == n * tokens
    span = fast * tokens

    def mix_side(f):
        if keep:

            @pl.loop(0, slow)
            def _(b):
                mix(b * fast + f, b * fast + f)

    def products(low, high):
        @pl.loop(low, high)
        def _(d):
            b = lax.rem(line - d + slow, slow)
            if not keep:
                for f in range(fast):
                    mix(b * fast + f, f)
            for f in range(fast):

                @pl.when((d > 0) | (f > 0))
                def _():
                    for j in range(1, nt):
                        onward(j, d * fast + f, lax.rem(ti - j + nt, nt)).wait_recv()

            term = jnp.dot(
                dy_in[:, aligned(b * span, span)],
                mixed[aligned(b * span, span), :] if keep else mixed[...],
                preferred_element_type=jnp.float32,
            )

            @pl.when(d == 0)
            def _():
                out_ref[...] = term

            @pl.when(d > 0)
            def _():
                out_ref[...] += term

    def own_rows():
        dy_in[:, aligned(me * tokens, tokens)] = turned[aligned(me * rows, rows, 8), :]

    def value_final():
        value_ref[...] = near_sum[line].astype(jnp.float32)

        if slow > 1:
            value_all.wait_recv()

        @pl.loop(1, slow)
        def _(k):
            value_ref[...] += value_in[k].astype(jnp.float32)

    @pl.when(last)
    def _():
        for j in range(per_part):
            upstream(ti, j, lambda s, at: head[s, at, :])
        turn(ti)
        mixed_grad(ti)
        values_grad(ti, mg_half, 0)
        relay((0, 1), 1, min(2, slow))
        turn_wv()
        relay((0, 1), min(2, slow), min(3, slow))
        send_dy()
        for i in range(1, nt):
            half = lax.rem(ti - i + nt, nt)
            for j in range(per_part):
                head_copy(i, j).wait_recv()
                upstream(half, j, lambda s, at: head_in[i, s, at, :])
            turn(half)
            mixed_grad(half)
            values_grad(half, mg_half, 0)
        for k in range(1, nt):
            wv_direct(k, 1).start()
        value_part()
        relay((0, 1), min(3, slow), slow)
        for k in range(1, nt):
            wv_direct(k, 1).wait_send()
        go_on()
        wv_arrive(True)
        norm_backward()
        pass_turn()
        pass_on(1, n)
        gain_sums()
        pack_waits()
        own_rows()
        for f in range(fast):
            mix_side(f)
        products(0, min(2, slow))
        near_sums()
        products(min(2, slow), slow)
        value_final()

    if np_ > 1:

        @pl.when(jnp.logical_not(last))
        def _():
            relay((0, 1), 1, slow)
            mix_side(side)
            turn_wv()
            pl.semaphore_wait(go, 1)
            wv_start(False)
            for i in range(nt):
                half = lax.rem(ti + i, nt)
                down_half(half).wait_recv()
                turn(half)
                if i == 0:
                    send_dy()
            wv_arrive(False)
            pl.semaphore_signal(back, inc=1, device_id={"pipe": pi + 1}, device_id_type=MESH)
            mixed_grad(None)
            for i in range(nt):
                values_grad(i, mg, i * part)
            value_part()
            pass_on(1, min(4, n))
            pack_waits()
            own_rows()
            for f in range(1, fast):
                mix_side(lax.rem(side + f, fast))
            pass_on(min(4, n), n)
            gain_sums()
            go_on()
            wv_wait()
            norm_backward()
            pass_turn()
            near_sums()
            products(0, slow)
            value_final()

    gain_sum = gx[me]
    gain_all.wait_recv()
    for k in range(1, n):
        gain_sum = gain_sum + gx_in[k]
    gain_out_ref[...] = gain_sum

    bound_all.wait_send()
    dy_all.wait_send()
    gain_all.wait_send()
    for j in range(1, nt):
        both_ends(
            dy_in.at[:, pl.ds(0, (n - 1) * part)], o_send.at[j - 1], o_recv.at[j - 1, 0]
        ).wait_send()
    if slow > 1:
        value_all.wait_send()
    if fast > 1:
        near_all.wait_send()
        y_all.wait_send()

    @pl.loop(0, slow)
    def _(b):
        for q in range(2):

            @pl.when((line < slow - 1) & (b <= line))
            def _():
                right_copy(q, b).wait_send()

            @pl.when((line > 0) & (b >= line))
            def _():
                left_copy(q, b).wait_send()

    for k in range(1, nt):
        gain_across(k).wait_send()
        for half in range(nt):

            @pl.when((pi > 0) | (half == lax.rem(ti + k, nt)))
            def _():
                vg_copy(k, half).wait_send()

    @pl.when(last)
    def _():
        wv_sent(True)
        for k in range(1, nt):
            for j in range(per_part):
                head_copy(k, j).wait_send()

    if np_ > 1:

        @pl.when(jnp.logical_not(last))
        def _():
            wv_sent(False)

    if np_ > 1:

        @pl.when(pi > 0)
        def _():
            for half in range(nt):
                down_half(half).wait_send()


def layer(sizes, hidden, probs, gain, wv, wo, head, policy, refer, bounds):
    n, nt, _ = sizes
    micro, both, length, width = hidden.shape
    own = head.shape[1]
    tokens = micro * both * length
    sequences = micro * both
    columns = wo.shape[0]
    heads = columns // LANES
    wcols = wv.shape[1]
    rows = width // n
    part = tokens // nt
    fast = 2 if n % 2 == 0 else 1
    slow = n // fast
    pack_rows = (
        len(bands(sequences, length)) * heads * BAND + wcols // LANES * tokens
    )
    per_part = part // length
    keep = n * tokens * columns <= 2**22
    vmem = pl.BlockSpec(memory_space=pltpu.VMEM)
    dma = pltpu.SemaphoreType.DMA
    bf, f32, i32 = jnp.bfloat16, jnp.float32, jnp.int32
    return pl.pallas_call(
        functools.partial(layer_kernel, sizes),
        out_shape=(
            pltpu.VMEM((micro, own, length, width), bf),
            pltpu.VMEM((rows, wcols), f32),
            pltpu.VMEM((rows, columns), f32),
            pltpu.VMEM((1, rows), f32),
        ),
        in_specs=[pl.BlockSpec(memory_space=pl.ANY)] * 9,
        out_specs=(vmem,) * 4,
        scratch_shapes=[
            pltpu.VMEM((tokens, width), bf),
            pltpu.VMEM((sequences, heads * length, length), bf),
            pltpu.VMEM((1, width), f32),
            pltpu.VMEM((width, nt * wcols), bf),
            pltpu.VMEM((columns, width), bf),
            pltpu.VMEM((own * micro, length, width), bf),
            pltpu.VMEM((nt, own * micro, length, width), bf),
            pltpu.VMEM(policy.shape, f32),
            pltpu.VMEM(refer.shape, f32),
            pltpu.VMEM(bounds.shape, i32),
            pltpu.VMEM((n,) + bounds.shape, i32),
            pltpu.VMEM((tokens, 1), f32),
            pltpu.VMEM((tokens, width), bf),
            pltpu.VMEM((tokens, 1), f32),
            pltpu.VMEM((n, pack_rows, LANES), bf),
            pltpu.VMEM((tokens, width), bf),
            pltpu.VMEM((width, tokens), bf),
            pltpu.VMEM((columns, tokens), bf),
            pltpu.VMEM((columns, part), bf),
            pltpu.VMEM((wcols, tokens), bf),
            pltpu.VMEM((tokens, nt * wcols), bf),
            pltpu.VMEM((part, width), f32),
            pltpu.VMEM((tokens, width), bf),
            pltpu.VMEM((width, wcols), bf),
            pltpu.VMEM((slow, rows, wcols), bf),
            pltpu.VMEM((slow, rows, wcols), bf),
            pltpu.VMEM((slow, rows, wcols), bf),
            pltpu.VMEM((rows, n * tokens), bf),
            pltpu.VMEM(((n if keep else fast) * tokens, columns), bf),
            pltpu.VMEM((wcols, width), bf),
            pltpu.VMEM((1, width), f32),
            pltpu.VMEM((nt, 1, width), f32),
            pltpu.VMEM((n, 1, rows), f32),
            pltpu.VMEM((n, 1, rows), f32),
            dma((6 + own * micro,)),
            dma((1,)),
            dma((1,)),
            dma((1,)),
            dma((1,)),
            dma((nt - 1, own * micro)),
            dma((nt - 1, own * micro)),
            dma((nt - 1, 2)),
            dma((nt - 1, 2)),
            dma((nt - 1,)),
            dma((nt - 1,)),
            dma((2, slow)),
            dma((2, slow)),
            dma((2, slow)),
            dma((1,)),
            dma((1,)),
            dma((1,)),
            dma((n - 1,)),
            dma((nt - 1,)),
            dma((nt - 1, n - 1)),
            dma((nt - 1, nt)),
            dma((nt - 1, nt)),
            dma((nt,)),
            dma((nt,)),
            dma((1,)),
            dma((slow,)),
            dma((1,)),
            dma((1,)),
            dma((1,)),
            dma((1,)),
            dma((nt - 1,)),
            dma((nt - 1,)),
            pltpu.SemaphoreType.REGULAR,
            pltpu.SemaphoreType.REGULAR,
        ],
        compiler_params=pltpu.CompilerParams(
            collective_id=0, has_side_effects=True, vmem_limit_bytes=52 * 2**20
        ),
        name="layer",
    )(hidden, probs, gain, wv, wo, head, policy, refer, bounds)


def finish_kernel(*refs):
    count = len(refs) // 2
    sem = refs[-1]
    copies = [
        pltpu.make_async_copy(refs[i], refs[count + i], sem.at[i]) for i in range(count)
    ]
    for copy in copies:
        copy.start()
    for copy in copies:
        copy.wait()


def finish(arrays):
    return pl.pallas_call(
        finish_kernel,
        out_shape=tuple(jax.ShapeDtypeStruct(a.shape, a.dtype) for a in arrays),
        in_specs=[pl.BlockSpec(memory_space=pltpu.VMEM)] * len(arrays),
        out_specs=(pl.BlockSpec(memory_space=pl.ANY),) * len(arrays),
        scratch_shapes=[pltpu.SemaphoreType.DMA((len(arrays),))],
        compiler_params=pltpu.CompilerParams(vmem_limit_bytes=2**20),
        name="finish",
    )(*(pltpu.with_memory_space_constraint(a, pltpu.VMEM) for a in arrays))


def body(
    hidden_in,
    attention_probs,
    norm_gain,
    value_weight,
    output_weight,
    head_grad,
    policy_logprob,
    reference_logprob,
    sequence_bounds,
):
    sizes = tuple(lax.axis_size(a) for a in ("dp", "tensor", "pipe"))
    micro, both, heads, length, _ = attention_probs.shape[1:]
    cotangent, value, output, gain = finish(layer(
        sizes,
        hidden_in[0],
        attention_probs[0].reshape(micro, both, heads * length, length),
        norm_gain,
        value_weight[0],
        output_weight[0],
        head_grad,
        policy_logprob,
        reference_logprob,
        sequence_bounds,
    ))
    return (cotangent[None], value[None], output[None], gain)


def solution(mesh):
    in_specs = (
        P("pipe", "dp", None, None, None),
        P("pipe", "dp", None, "tensor", None, None),
        P("pipe", None),
        P("pipe", None, "tensor"),
        P("pipe", "tensor", None),
        P("dp", "tensor", None, None),
        P("dp", None, None),
        P("dp", None),
        P("dp", None),
    )
    out_specs = (
        P("pipe", "dp", "tensor", None, None),
        P("pipe", "dp", "tensor"),
        P("pipe", "dp", "tensor"),
        P("pipe", "dp"),
    )
    return jax.shard_map(body, mesh=mesh, in_specs=in_specs, out_specs=out_specs, check_vma=False)
```

```python
import functools

import jax
import jax.numpy as jnp
from jax import lax
from jax.experimental import pallas as pl
from jax.experimental.pallas import tpu as pltpu
from jax.sharding import PartitionSpec as P

LANES = 128
BAND = 16
MESH = pl.DeviceIdType.MESH

EPSILON = 1e-06
DPO_BETA = 0.25
LIKELIHOOD_COEF = 0.2


def greet(peers):
    barrier = pltpu.get_barrier_semaphore()
    total = 0
    for axis, n in peers:
        me = lax.axis_index(axis)

        @pl.loop(1, n)
        def _(k):
            pl.semaphore_signal(
                barrier, inc=1, device_id={axis: lax.rem(me + k, n)}, device_id_type=MESH
            )

        total += n - 1
    pl.semaphore_wait(barrier, total)


def remote(src, dst, send_sem, recv_sem, **device):
    return pltpu.make_async_remote_copy(
        src_ref=src,
        dst_ref=dst,
        send_sem=send_sem,
        recv_sem=recv_sem,
        device_id=device,
        device_id_type=MESH,
    )


def aligned(start, size, to=None):
    return pl.ds(pl.multiple_of(start, to or size), size)


def bands(sequences, length):
    todo = sorted(
        ((b + 1) * BAND, b, s) for b in range(length // BAND) for s in range(sequences)
    )
    groups = []
    for width, b, s in sorted(todo, key=lambda t: (-t[0], t[2])):
        for group in groups:
            start = sum(w for w, _, _ in group)
            if start + width <= LANES:
                group.append((width, b, s))
                break
        else:
            groups.append([(width, b, s)])
    return groups


def layer_kernel(
    sizes,
    hidden_hbm,
    probs_hbm,
    gain_hbm,
    wv_hbm,
    wo_hbm,
    head_hbm,
    policy_hbm,
    refer_hbm,
    bounds_hbm,
    cot_ref,
    value_ref,
    out_ref,
    gain_out_ref,
    hid,
    prob,
    gain,
    wvc,
    wo,
    head,
    head_in,
    policy,
    refer,
    bound,
    bound_in,
    wcol,
    normed,
    rms,
    packs,
    dy,
    turned,
    mg,
    mg_half,
    vgt,
    vgc,
    ng,
    rows_ref,
    vpart,
    near_in,
    near_sum,
    value_in,
    dy_in,
    mixed,
    wvt,
    gt,
    gt_in,
    gx,
    gx_in,
    load_sem,
    h_load,
    p_load,
    b_send,
    b_recv,
    h_send,
    h_recv,
    w_send,
    w_recv,
    a_send,
    a_recv,
    r_send,
    l_send,
    z_recv,
    y_send,
    y_recv,
    d_send,
    d_recv,
    o_send,
    o_recv,
    v_send,
    v_recv,
    c_send,
    c_recv,
    n_send,
    n_recv,
    s_send,
    s_recv,
    g_send,
    g_recv,
    t_send,
    t_recv,
    go,
    back,
):
    n, nt, np_ = sizes
    me, ti, pi = lax.axis_index("dp"), lax.axis_index("tensor"), lax.axis_index("pipe")
    micro, both, length, width = hidden_hbm.shape
    own = head_hbm.shape[1]
    tokens = micro * both * length
    part = tokens // nt
    per_part = part // length
    columns = wo.shape[0]
    heads = columns // LANES
    wcols = wv_hbm.shape[1]
    value_heads = wcols // LANES
    per_value = heads // value_heads
    rows = width // n
    fast = 2 if n % 2 == 0 else 1
    slow = n // fast
    line, side = lax.div(me, fast), lax.rem(me, fast)
    partner = me + 1 - 2 * side
    last = pi == np_ - 1
    groups = bands(micro * both, length)
    group_rows = heads * BAND
    value_base = len(groups) * group_rows
    pack_parts = ((0, value_base), (value_base, tokens * value_heads))

    def load(src, dst, i):
        return pltpu.make_async_copy(src, dst, load_sem.at[i])

    mine = aligned(ti * wcols, wcols)
    small = [
        load(bounds_hbm, bound, 0),
        load(policy_hbm, policy, 1),
        load(refer_hbm, refer, 2),
        load(gain_hbm, gain, 3),
    ]
    wv_load = load(wv_hbm, wvc.at[:, mine], 4)
    wo_load = load(wo_hbm, wo, 5)
    hid_loads, prob_loads, head_loads = [], [], []
    for c in range(both):
        for p in range(micro):
            s = c * micro + p
            hid_loads.append(
                pltpu.make_async_copy(
                    hidden_hbm.at[p, c], hid.at[pl.ds(s * length, length)], h_load.at[0]
                )
            )
            prob_loads.append(
                pltpu.make_async_copy(probs_hbm.at[p, c], prob.at[s], p_load.at[0])
            )
    for o in range(own):
        for p in range(micro):
            head_loads.append(load(head_hbm.at[p, o], head.at[o * micro + p], 6 + o * micro + p))
    small[0].start()

    @pl.when(last)
    def _():
        for copy in head_loads:
            copy.start()

    for copy in hid_loads + small[1:]:
        copy.start()
    wv_load.start()
    for copy in prob_loads:
        copy.start()
    wo_load.start()
    greet((("dp", n), ("tensor", nt), ("pipe", np_)))

    def both_ends(block, send, recv):
        return remote(block, block, send, recv, dp=lax.rem(me + 1, n))

    def bound_copy(k):
        return remote(bound, bound_in.at[k], b_send.at[0], b_recv.at[0], dp=lax.rem(me + k, n))

    bound_all = both_ends(bound_in.at[pl.ds(1, n - 1)], b_send.at[0], b_recv.at[0])

    def head_copy(k, j):
        return remote(
            head.at[j], head_in.at[k, j], h_send.at[k - 1, j], h_recv.at[k - 1, j],
            tensor=lax.rem(ti + k, nt),
        )

    quarter = width // 4

    def wv_copy(k, piece):
        block = wvc.at[aligned(piece * quarter, quarter, BAND), mine]
        return remote(
            block, block, w_send.at[k - 1, 1], w_recv.at[k - 1, 1], tensor=lax.rem(ti + k, nt)
        )

    def wv_other(k):
        return wvc.at[pl.ds(0, width // 2), aligned(lax.rem(ti - k + nt, nt) * wcols, wcols)]

    def wv_direct(k, i):
        block = wvc.at[pl.ds(*((0, 3 * quarter), (3 * quarter, quarter))[i]), mine]
        return remote(
            block, block, w_send.at[k - 1, i], w_recv.at[k - 1, i], tensor=lax.rem(ti + k, nt)
        )

    def wv_across(k, piece):
        at = aligned(lax.rem(ti - k + nt, nt) * wcols, wcols)
        block = wvc.at[aligned(piece * quarter, quarter, BAND), at]
        return remote(block, block, a_send.at[k - 1], a_recv.at[k - 1], dp=partner)

    def wv_half(k):
        return remote(
            wv_other(k), wv_other(k), w_send.at[k - 1, 1], w_recv.at[k - 1, 1],
            tensor=lax.rem(ti + k, nt),
        )

    pieces = (side, 2 + side)

    def wv_start(direct):
        for k in range(1, nt):
            if direct or fast == 1:
                wv_direct(k, 0).start()
                if not direct:
                    wv_direct(k, 1).start()
            else:
                for piece in pieces:
                    wv_copy(k, piece).start()

    def wv_arrive(direct):
        for k in range(1, nt):
            if direct or fast == 1:
                wv_direct(k, 0).wait_recv()
                wv_direct(k, 1).wait_recv()
            else:
                wv_half(k).wait_recv()
                for piece in pieces:
                    wv_across(k, piece).start()

    def wv_across_all(k):
        return both_ends(wv_other(k), a_send.at[k - 1], a_recv.at[k - 1])

    def wv_wait():
        if fast > 1:
            for k in range(1, nt):
                wv_across_all(k).wait_recv()

    def wv_sent(direct):
        for k in range(1, nt):
            if direct or fast == 1:
                wv_direct(k, 0).wait_send()
                if not direct:
                    wv_direct(k, 1).wait_send()
            else:
                wv_half(k).wait_send()
                wv_across_all(k).wait_send()

    def pass_turn():
        if np_ > 1:

            @pl.when(pi > 0)
            def _():
                pl.semaphore_wait(back, 1)

    def go_on():
        if np_ > 1:

            @pl.when(pi > 0)
            def _():
                pl.semaphore_signal(go, inc=1, device_id={"pipe": pi - 1}, device_id_type=MESH)

    def vg_copy(k, half):
        block = vgc.at[aligned(half * part, part), mine]
        return remote(
            block, block, v_send.at[k - 1, half], v_recv.at[k - 1, half], tensor=lax.rem(ti + k, nt)
        )

    def pack_copy(q, b, send, peer):
        block = packs.at[b * fast + side, pl.ds(*pack_parts[q])]
        return remote(block, block, send.at[q, b], z_recv.at[q, b], dp=peer)

    def right_copy(q, b):
        return pack_copy(q, b, r_send, lax.rem(me + fast, n))

    def left_copy(q, b):
        return pack_copy(q, b, l_send, lax.rem(me - fast + n, n))

    def y_copy(q, b):
        block = packs.at[b * fast + side, pl.ds(*pack_parts[q])]
        return remote(block, block, y_send.at[0], y_recv.at[0], dp=partner)

    y_all = both_ends(packs.at[pl.ds(0, slow)], y_send.at[0], y_recv.at[0])

    def send_pack(q, b):
        @pl.when((line < slow - 1) & (b <= line))
        def _():
            right_copy(q, b).start()

        @pl.when((line > 0) & (b >= line))
        def _():
            left_copy(q, b).start()

        if fast > 1:
            y_copy(q, b).start()

    def relay(parts, low, high):
        @pl.loop(low, high)
        def _(d):
            for q in parts:

                @pl.when(line >= d)
                def _():
                    right_copy(q, line - d).wait_recv()
                    send_pack(q, line - d)

                @pl.when(line + d < slow)
                def _():
                    left_copy(q, line + d).wait_recv()
                    send_pack(q, line + d)

    def ahead(e):
        d, f = lax.div(e, fast), lax.rem(e, fast)
        there = lax.rem(line + d, slow) * fast + lax.rem(side + f, fast)
        back = lax.rem(line - d + slow, slow) * fast + lax.rem(side - f + fast, fast)
        return there, back

    def dy_copy(e):
        peer = ahead(e)[0]
        return remote(
            turned.at[aligned(peer * rows, rows, 8), aligned(ti * part, part)],
            dy_in.at[:, aligned(me * tokens + ti * part, part)],
            d_send.at[0], d_recv.at[e - 1], dp=peer,
        )

    def onward(j, e, half):
        block = dy_in.at[:, aligned(ahead(e)[1] * tokens + half * part, part)]
        return remote(
            block, block, o_send.at[j - 1], o_recv.at[j - 1, e - 1], tensor=lax.rem(ti + j, nt)
        )

    def down_copy(half, j):
        at = aligned(half * part + j * length, length)
        return remote(
            rows_ref.at[at], dy.at[at], c_send.at[half], c_recv.at[half],
            pipe=lax.rem(pi - 1 + np_, np_),
        )

    def down_half(half):
        at = half_of(half)
        return remote(
            rows_ref.at[at], dy.at[at], c_send.at[half], c_recv.at[half],
            pipe=lax.rem(pi - 1 + np_, np_),
        )

    def near_copy(j):
        block = j * fast + fast - 1 - side
        return remote(
            vpart.at[aligned(block * rows, rows, 8)], near_in.at[j], n_send.at[0], n_recv.at[j],
            dp=partner,
        )

    def value_copy(k):
        return remote(
            near_sum.at[lax.rem(line + k, slow)], value_in.at[k], s_send.at[0], s_recv.at[0],
            dp=lax.rem(me + fast * k, n),
        )

    def gain_across(k):
        return remote(gt, gt_in.at[k], t_send.at[k - 1], t_recv.at[k - 1], tensor=lax.rem(ti + k, nt))

    def gain_copy(k):
        peer = lax.rem(me + k, n)
        return remote(gx.at[peer], gx_in.at[k], g_send.at[0], g_recv.at[0], dp=peer)

    gain_all = both_ends(gx_in.at[pl.ds(1, n - 1)], g_send.at[0], g_recv.at[0])
    dy_all = both_ends(
        dy_in.at[:, pl.ds(0, (n - 1) * part)], d_send.at[0], d_recv.at[0]
    )
    near_all = both_ends(near_in, n_send.at[0], n_recv.at[0])
    value_all = both_ends(value_in.at[pl.ds(0, max(1, slow - 1))], s_send.at[0], s_recv.at[0])

    small[0].wait()

    @pl.loop(1, n)
    def _(k):
        bound_copy(k).start()

    @pl.when(last)
    def _():
        for j in range(per_part):
            head_loads[j].wait()
            for k in range(1, nt):
                head_copy(k, j).start()

    wv_load.wait()

    @pl.when(last)
    def _():
        wv_start(True)

    pltpu.make_async_copy(prob, prob, p_load.at[0]).wait()
    for i, group in enumerate(groups):
        for h in range(heads):
            row = h * length
            cells = [
                prob[s, row + b * BAND : row + (b + 1) * BAND, 0:w] for w, b, s in group
            ]
            spare = LANES - sum(w for w, _, _ in group)
            if spare:
                cells.append(jnp.zeros((BAND, spare), jnp.bfloat16))
            first = i * group_rows + h * BAND
            packs[me, first : first + BAND, :] = jnp.concatenate(cells, axis=1)
    send_pack(0, line)

    def half_of(half):
        return aligned(half * part, part)

    def upstream(half, j, block):
        @pl.loop(0, length // BAND)
        def _(r):
            to = aligned(half * part + j * length + r * BAND, BAND)
            rows_in = block(j, aligned(r * BAND, BAND))
            dy[to, :] = (wcol[to, :] * rows_in.astype(jnp.float32)).astype(jnp.bfloat16)

    lots = next(c for c in (4, 2, 1) if width // LANES % c == 0)

    def turn(half):
        at = half_of(half)

        @pl.loop(0, width // (LANES * lots))
        def _(j):
            for i in range(lots):
                to = aligned((j * lots + i) * LANES, LANES)
                turned[to, at] = dy[at, to].T

    def send_dy():
        @pl.loop(1, n)
        def _(k):
            dy_copy(k).start()

    def values_grad(half, source, base):
        at = half_of(half)
        for v in range(value_heads):
            across = []
            for j in range(per_part):
                stacked = jnp.concatenate(
                    [
                        source[
                            h * LANES : (h + 1) * LANES,
                            base + j * length : base + (j + 1) * length,
                        ]
                        for h in range(v * per_value, (v + 1) * per_value)
                    ],
                    axis=1,
                )
                pattern = prob[
                    half * per_part + j, v * per_value * length : (v + 1) * per_value * length, :
                ]
                across.append(jnp.dot(stacked, pattern, preferred_element_type=jnp.float32))
            block = jnp.concatenate(across, axis=1)
            vgt[v * LANES : (v + 1) * LANES, at] = block.astype(jnp.bfloat16)
            vgc[at, aligned(ti * wcols + v * LANES, LANES)] = block.T.astype(jnp.bfloat16)
        for k in range(1, nt):

            @pl.when((pi > 0) | (half == lax.rem(ti + k, nt)))
            def _():
                vg_copy(k, half).start()

    def mixed_grad(half):
        if half is None:
            mg[...] = jnp.dot(wo[...], turned[...], preferred_element_type=jnp.float32).astype(
                jnp.bfloat16
            )
        else:
            for i in range(nt):

                @pl.when(half == i)
                def _():
                    mg_half[...] = jnp.dot(
                        wo[...],
                        turned[:, i * part : (i + 1) * part],
                        preferred_element_type=jnp.float32,
                    ).astype(jnp.bfloat16)

    def pass_on(low, high):
        @pl.loop(low, high)
        def _(k):
            dy_copy(k).wait_recv()
            for j in range(1, nt):
                onward(j, k, ti).start()

    def norm_backward(between=0):
        @pl.loop(0, nt)
        def _(i):
            half = lax.rem(ti + i, nt)

            @pl.when((i == 0) | (pi > 0))
            def _():
                for k in range(1, nt):
                    vg_copy(k, half).wait_recv()
                ng[...] = lax.dot_general(
                    vgc[half_of(half), :],
                    wvc[...],
                    (((1,), (1,)), ((), ())),
                    preferred_element_type=jnp.float32,
                )
                for j in range(per_part):

                    @pl.loop(0, length // BAND)
                    def _(r):
                        here = aligned(j * length + r * BAND, BAND)
                        to = aligned(half * part + j * length + r * BAND, BAND)
                        x = hid[to, :].astype(jnp.float32)
                        inverse = rms[to, :]
                        scaled = ng[here, :] * gain[...]
                        mean = jnp.mean(x * scaled, axis=-1, keepdims=True)
                        grad = inverse * scaled - x * (inverse * inverse * inverse * mean)
                        rows_ref[to, :] = (dy[to, :].astype(jnp.float32) + grad).astype(
                            jnp.bfloat16
                        )

                    if np_ > 1:

                        @pl.when(pi > 0)
                        def _():
                            down_copy(half, j).start()

                if between:

                    @pl.when(i == 0)
                    def _():
                        pass_on(1, between)


        for o in range(own):
            for p in range(micro):
                cot_ref[p, o] = rows_ref[aligned(ti * part + (o * micro + p) * length, length), :]

    def gain_sums():
        whole = gt[...]
        for k in range(1, nt):
            gain_across(k).wait_recv()
            whole = whole + gt_in[k]
        for i in range(n):
            gx[i] = whole[:, i * rows : (i + 1) * rows]

        @pl.loop(1, n)
        def _(k):
            gain_copy(k).start()

    for copy in small[1:]:
        copy.wait()
    pltpu.make_async_copy(hid, hid, h_load.at[0]).wait()

    @pl.loop(0, tokens // BAND)
    def _(i):
        at = aligned(i * BAND, BAND)
        x = hid[at, :].astype(jnp.float32)
        inverse = lax.rsqrt(jnp.mean(x * x, axis=-1, keepdims=True) + EPSILON)
        rms[at, :] = inverse
        normed[at, :] = (x * inverse * gain[...]).astype(jnp.bfloat16)

    values = jnp.dot(normed[...], wvc[:, mine], preferred_element_type=jnp.float32).astype(
        jnp.bfloat16
    )
    for v in range(value_heads):
        packs[me, value_base + v * tokens : value_base + (v + 1) * tokens, :] = values[
            :, v * LANES : (v + 1) * LANES
        ]
    send_pack(1, line)
    wo_load.wait()

    def responses(b):
        spans = jnp.minimum(b[:, 1:2], length) - jnp.maximum(b[:, 0:1], 0)
        return jnp.sum(jnp.maximum(spans, 0), axis=0, keepdims=True)

    total = responses(bound[...])
    bound_all.wait_recv()
    for k in range(1, n):
        total = total + responses(bound_in[k])
    likelihood = LIKELIHOOD_COEF * micro * n / total.astype(jnp.float32)
    along = lax.broadcasted_iota(jnp.int32, (1, length), 1)
    down = lax.broadcasted_iota(jnp.int32, (length, 1), 0)
    for p in range(micro):
        low = bound[p : p + 1, 0:1]
        scores = []
        for c in range(both):
            high = bound[p : p + 1, 1 + c : 2 + c]
            inside = jnp.where((along >= low) & (along < high), policy[p, c : c + 1, :], 0.0)
            scores.append(
                jnp.sum(inside, axis=-1, keepdims=True) - refer[p : p + 1, c : c + 1]
            )
        margin = DPO_BETA * (scores[0] - scores[1])
        pair = jax.nn.sigmoid(-margin)
        for c in range(both):
            high = bound[p : p + 1, 1 + c : 2 + c]
            weight = -DPO_BETA * pair - likelihood if c == 0 else DPO_BETA * pair
            inside = (down >= low) & (down < high)
            wcol[(c * micro + p) * length : (c * micro + p + 1) * length, :] = jnp.where(
                inside, jnp.broadcast_to(weight, (length, 1)), 0.0
            )

    def mix(src, slot):
        for v in range(value_heads):
            for i, group in enumerate(groups):
                first = i * group_rows + v * per_value * BAND
                pattern = packs[src, first : first + per_value * BAND, :]
                blocks, start = [], 0
                for w, b, s in group:
                    key = value_base + v * tokens + s * length
                    cells = [packs[src, key : key + w, :]]
                    if start:
                        cells.insert(0, jnp.zeros((start, LANES), jnp.bfloat16))
                    if start + w < LANES:
                        cells.append(jnp.zeros((LANES - start - w, LANES), jnp.bfloat16))
                    blocks.append(jnp.concatenate(cells, axis=0) if len(cells) > 1 else cells[0])
                    start += w
                product = jnp.dot(
                    pattern,
                    jnp.concatenate(blocks, axis=1) if len(blocks) > 1 else blocks[0],
                    preferred_element_type=jnp.float32,
                ).astype(jnp.bfloat16)
                for j, (w, b, s) in enumerate(group):
                    row = s * length + b * BAND
                    for h in range(per_value):
                        column = (v * per_value + h) * LANES
                        mixed[
                            aligned(slot * tokens + row, BAND), column : column + LANES
                        ] = product[
                            h * BAND : (h + 1) * BAND, j * LANES : (j + 1) * LANES
                        ]

    def turn_wv():
        @pl.loop(0, width // (LANES * lots))
        def _(j):
            for i in range(lots):
                to = aligned((j * lots + i) * LANES, LANES)
                wvt[:, to] = wvc[to, mine].T

    def value_part():
        for v in range(value_heads):
            ng[0:LANES, :] = jnp.dot(
                vgt[v * LANES : (v + 1) * LANES, :],
                normed[...],
                preferred_element_type=jnp.float32,
            )
            part_gain = jnp.sum(
                ng[0:LANES, :] * wvt[v * LANES : (v + 1) * LANES, :].astype(jnp.float32),
                axis=0,
                keepdims=True,
            )
            gt[...] = part_gain if v == 0 else gt[...] + part_gain

            @pl.loop(0, width // (LANES * lots))
            def _(j):
                for i in range(lots):
                    to = aligned((j * lots + i) * LANES, LANES)
                    vpart[to, v * LANES : (v + 1) * LANES] = (
                        ng[0:LANES, to].astype(jnp.bfloat16).T
                    )

        if fast > 1:

            @pl.loop(1, slow + 1)
            def _(k):
                near_copy(lax.rem(line + k, slow)).start()

        gt[...] = gt[...] / gain[...]
        for k in range(1, nt):
            gain_across(k).start()

    def near_sums():
        @pl.loop(1, slow + 1)
        def _(k):
            j = lax.rem(line + k, slow)
            near = vpart[aligned((j * fast + side) * rows, rows, 8), :].astype(jnp.float32)
            if fast > 1:
                near_copy(j).wait_recv()
                near = near + near_in[j].astype(jnp.float32)
            near_sum[j] = near.astype(jnp.bfloat16)

            @pl.when(k < slow)
            def _():
                value_copy(k).start()

    def pack_waits():
        if fast > 1:

            y_all.wait_recv()

    keep = mixed.shape[0] == n * tokens
    span = fast * tokens

    def mix_side(f):
        if keep:

            @pl.loop(0, slow)
            def _(b):
                mix(b * fast + f, b * fast + f)

    def products(low, high):
        @pl.loop(low, high)
        def _(d):
            b = lax.rem(line - d + slow, slow)
            if not keep:
                for f in range(fast):
                    mix(b * fast + f, f)
            for f in range(fast):

                @pl.when((d > 0) | (f > 0))
                def _():
                    for j in range(1, nt):
                        onward(j, d * fast + f, lax.rem(ti - j + nt, nt)).wait_recv()

            term = jnp.dot(
                dy_in[:, aligned(b * span, span)],
                mixed[aligned(b * span, span), :] if keep else mixed[...],
                preferred_element_type=jnp.float32,
            )

            @pl.when(d == 0)
            def _():
                out_ref[...] = term

            @pl.when(d > 0)
            def _():
                out_ref[...] += term

    def own_rows():
        dy_in[:, aligned(me * tokens, tokens)] = turned[aligned(me * rows, rows, 8), :]

    def value_final():
        value_ref[...] = near_sum[line].astype(jnp.float32)

        if slow > 1:
            value_all.wait_recv()

        @pl.loop(1, slow)
        def _(k):
            value_ref[...] += value_in[k].astype(jnp.float32)

    @pl.when(last)
    def _():
        for j in range(per_part):
            upstream(ti, j, lambda s, at: head[s, at, :])
        turn(ti)
        mixed_grad(ti)
        values_grad(ti, mg_half, 0)
        relay((0, 1), 1, min(2, slow))
        turn_wv()
        relay((0, 1), min(2, slow), min(3, slow))
        for i in range(1, nt):
            half = lax.rem(ti - i + nt, nt)
            for j in range(per_part):
                head_copy(i, j).wait_recv()
                upstream(half, j, lambda s, at: head_in[i, s, at, :])
            turn(half)
            if i == 1:
                send_dy()
            mixed_grad(half)
            values_grad(half, mg_half, 0)
        for k in range(1, nt):
            wv_direct(k, 1).start()
        value_part()
        relay((0, 1), min(3, slow), slow)
        for k in range(1, nt):
            wv_direct(k, 1).wait_send()
        go_on()
        wv_arrive(True)
        norm_backward()
        pass_turn()
        pass_on(1, n)
        gain_sums()
        pack_waits()
        own_rows()
        for f in range(fast):
            mix_side(f)
        products(0, min(2, slow))
        near_sums()
        products(min(2, slow), slow)
        value_final()

    if np_ > 1:

        @pl.when(jnp.logical_not(last))
        def _():
            relay((0, 1), 1, slow)
            mix_side(side)
            turn_wv()
            pl.semaphore_wait(go, 1)
            wv_start(False)
            for i in range(nt):
                half = lax.rem(ti + i, nt)
                down_half(half).wait_recv()
                turn(half)
                if i == 0:
                    send_dy()
            wv_arrive(False)
            pl.semaphore_signal(back, inc=1, device_id={"pipe": pi + 1}, device_id_type=MESH)
            mixed_grad(None)
            for i in range(nt):
                values_grad(i, mg, i * part)
            value_part()
            pass_on(1, min(4, n))
            pack_waits()
            own_rows()
            for f in range(1, fast):
                mix_side(lax.rem(side + f, fast))
            pass_on(min(4, n), n)
            gain_sums()
            go_on()
            wv_wait()
            norm_backward()
            pass_turn()
            near_sums()
            products(0, slow)
            value_final()

    gain_sum = gx[me]
    gain_all.wait_recv()
    for k in range(1, n):
        gain_sum = gain_sum + gx_in[k]
    gain_out_ref[...] = gain_sum

    bound_all.wait_send()
    dy_all.wait_send()
    gain_all.wait_send()
    for j in range(1, nt):
        both_ends(
            dy_in.at[:, pl.ds(0, (n - 1) * part)], o_send.at[j - 1], o_recv.at[j - 1, 0]
        ).wait_send()
    if slow > 1:
        value_all.wait_send()
    if fast > 1:
        near_all.wait_send()
        y_all.wait_send()

    @pl.loop(0, slow)
    def _(b):
        for q in range(2):

            @pl.when((line < slow - 1) & (b <= line))
            def _():
                right_copy(q, b).wait_send()

            @pl.when((line > 0) & (b >= line))
            def _():
                left_copy(q, b).wait_send()

    for k in range(1, nt):
        gain_across(k).wait_send()
        for half in range(nt):

            @pl.when((pi > 0) | (half == lax.rem(ti + k, nt)))
            def _():
                vg_copy(k, half).wait_send()

    @pl.when(last)
    def _():
        wv_sent(True)
        for k in range(1, nt):
            for j in range(per_part):
                head_copy(k, j).wait_send()

    if np_ > 1:

        @pl.when(jnp.logical_not(last))
        def _():
            wv_sent(False)

    if np_ > 1:

        @pl.when(pi > 0)
        def _():
            for half in range(nt):
                down_half(half).wait_send()


def layer(sizes, hidden, probs, gain, wv, wo, head, policy, refer, bounds):
    n, nt, _ = sizes
    micro, both, length, width = hidden.shape
    own = head.shape[1]
    tokens = micro * both * length
    sequences = micro * both
    columns = wo.shape[0]
    heads = columns // LANES
    wcols = wv.shape[1]
    rows = width // n
    part = tokens // nt
    fast = 2 if n % 2 == 0 else 1
    slow = n // fast
    pack_rows = (
        len(bands(sequences, length)) * heads * BAND + wcols // LANES * tokens
    )
    per_part = part // length
    keep = n * tokens * columns <= 2**22
    vmem = pl.BlockSpec(memory_space=pltpu.VMEM)
    dma = pltpu.SemaphoreType.DMA
    bf, f32, i32 = jnp.bfloat16, jnp.float32, jnp.int32
    return pl.pallas_call(
        functools.partial(layer_kernel, sizes),
        out_shape=(
            pltpu.VMEM((micro, own, length, width), bf),
            pltpu.VMEM((rows, wcols), f32),
            pltpu.VMEM((rows, columns), f32),
            pltpu.VMEM((1, rows), f32),
        ),
        in_specs=[pl.BlockSpec(memory_space=pl.ANY)] * 9,
        out_specs=(vmem,) * 4,
        scratch_shapes=[
            pltpu.VMEM((tokens, width), bf),
            pltpu.VMEM((sequences, heads * length, length), bf),
            pltpu.VMEM((1, width), f32),
            pltpu.VMEM((width, nt * wcols), bf),
            pltpu.VMEM((columns, width), bf),
            pltpu.VMEM((own * micro, length, width), bf),
            pltpu.VMEM((nt, own * micro, length, width), bf),
            pltpu.VMEM(policy.shape, f32),
            pltpu.VMEM(refer.shape, f32),
            pltpu.VMEM(bounds.shape, i32),
            pltpu.VMEM((n,) + bounds.shape, i32),
            pltpu.VMEM((tokens, 1), f32),
            pltpu.VMEM((tokens, width), bf),
            pltpu.VMEM((tokens, 1), f32),
            pltpu.VMEM((n, pack_rows, LANES), bf),
            pltpu.VMEM((tokens, width), bf),
            pltpu.VMEM((width, tokens), bf),
            pltpu.VMEM((columns, tokens), bf),
            pltpu.VMEM((columns, part), bf),
            pltpu.VMEM((wcols, tokens), bf),
            pltpu.VMEM((tokens, nt * wcols), bf),
            pltpu.VMEM((part, width), f32),
            pltpu.VMEM((tokens, width), bf),
            pltpu.VMEM((width, wcols), bf),
            pltpu.VMEM((slow, rows, wcols), bf),
            pltpu.VMEM((slow, rows, wcols), bf),
            pltpu.VMEM((slow, rows, wcols), bf),
            pltpu.VMEM((rows, n * tokens), bf),
            pltpu.VMEM(((n if keep else fast) * tokens, columns), bf),
            pltpu.VMEM((wcols, width), bf),
            pltpu.VMEM((1, width), f32),
            pltpu.VMEM((nt, 1, width), f32),
            pltpu.VMEM((n, 1, rows), f32),
            pltpu.VMEM((n, 1, rows), f32),
            dma((6 + own * micro,)),
            dma((1,)),
            dma((1,)),
            dma((1,)),
            dma((1,)),
            dma((nt - 1, own * micro)),
            dma((nt - 1, own * micro)),
            dma((nt - 1, 2)),
            dma((nt - 1, 2)),
            dma((nt - 1,)),
            dma((nt - 1,)),
            dma((2, slow)),
            dma((2, slow)),
            dma((2, slow)),
            dma((1,)),
            dma((1,)),
            dma((1,)),
            dma((n - 1,)),
            dma((nt - 1,)),
            dma((nt - 1, n - 1)),
            dma((nt - 1, nt)),
            dma((nt - 1, nt)),
            dma((nt,)),
            dma((nt,)),
            dma((1,)),
            dma((slow,)),
            dma((1,)),
            dma((1,)),
            dma((1,)),
            dma((1,)),
            dma((nt - 1,)),
            dma((nt - 1,)),
            pltpu.SemaphoreType.REGULAR,
            pltpu.SemaphoreType.REGULAR,
        ],
        compiler_params=pltpu.CompilerParams(
            collective_id=0, has_side_effects=True, vmem_limit_bytes=52 * 2**20
        ),
        name="layer",
    )(hidden, probs, gain, wv, wo, head, policy, refer, bounds)


def finish_kernel(*refs):
    count = len(refs) // 2
    sem = refs[-1]
    copies = [
        pltpu.make_async_copy(refs[i], refs[count + i], sem.at[i]) for i in range(count)
    ]
    for copy in copies:
        copy.start()
    for copy in copies:
        copy.wait()


def finish(arrays):
    return pl.pallas_call(
        finish_kernel,
        out_shape=tuple(jax.ShapeDtypeStruct(a.shape, a.dtype) for a in arrays),
        in_specs=[pl.BlockSpec(memory_space=pltpu.VMEM)] * len(arrays),
        out_specs=(pl.BlockSpec(memory_space=pl.ANY),) * len(arrays),
        scratch_shapes=[pltpu.SemaphoreType.DMA((len(arrays),))],
        compiler_params=pltpu.CompilerParams(vmem_limit_bytes=2**20),
        name="finish",
    )(*(pltpu.with_memory_space_constraint(a, pltpu.VMEM) for a in arrays))


def body(
    hidden_in,
    attention_probs,
    norm_gain,
    value_weight,
    output_weight,
    head_grad,
    policy_logprob,
    reference_logprob,
    sequence_bounds,
):
    sizes = tuple(lax.axis_size(a) for a in ("dp", "tensor", "pipe"))
    micro, both, heads, length, _ = attention_probs.shape[1:]
    cotangent, value, output, gain = finish(layer(
        sizes,
        hidden_in[0],
        attention_probs[0].reshape(micro, both, heads * length, length),
        norm_gain,
        value_weight[0],
        output_weight[0],
        head_grad,
        policy_logprob,
        reference_logprob,
        sequence_bounds,
    ))
    return (cotangent[None], value[None], output[None], gain)


def solution(mesh):
    in_specs = (
        P("pipe", "dp", None, None, None),
        P("pipe", "dp", None, "tensor", None, None),
        P("pipe", None),
        P("pipe", None, "tensor"),
        P("pipe", "tensor", None),
        P("dp", "tensor", None, None),
        P("dp", None, None),
        P("dp", None),
        P("dp", None),
    )
    out_specs = (
        P("pipe", "dp", "tensor", None, None),
        P("pipe", "dp", "tensor"),
        P("pipe", "dp", "tensor"),
        P("pipe", "dp"),
    )
    return jax.shard_map(body, mesh=mesh, in_specs=in_specs, out_specs=out_specs, check_vma=False)
```
